512 devices in a mesh: leaf: 32 (over z_hi, x, core), group: 16 (over y, z_lo).
Axes of the slice: x: 4, y: 4, z: 16 (z_hi: 4, z_lo: 4; z = z_hi * 4 + z_lo), core: 2. Of those that a mesh axis runs over, the one named last changes fastest.
Arguments:
- coefficients: float32 [16, 4096, 512], P('group', 'leaf'), may hold values from -6 to 6
- labels: float32 [16, 4096, 512], P('group', 'leaf'), may hold values from -6 to 6
- near_kernel: float32 [16, 4096, 3072], P('group', 'leaf'), may hold values from -0.109375 to 0.109375
- basis: float32 [16, 4096, 256], P('group', 'leaf'), may hold values from -0.1875 to 0.1875
- transfer: float32 [16, 1024, 256], P('group', 'leaf'), may hold values from -0.375 to 0.375
- coupling: float32 [16, 256, 4096], P('group', 'leaf'), may hold values from -0.09375 to 0.09375
- near_lists: int32 [16, 4, 3], P('group'), may hold values from 0 to 3, as said below
- ridge: float32 [1], replicated, may hold values from 0.5 to 2
Outputs:
- residual: float32 [16, 4096, 512], P('group', 'leaf')
The draws below stay inside these ranges and needn't reach their ends.
Inputs may be any that keep to these rules, and one draw needn't show every extreme that they name: `near_lists`: entry 0 of each leaf's list is the leaf itself; in each group the leaves lie on one cycle through all 4 leaves, and entries 1 and 2 of a leaf's list are its two neighbours on that cycle.
All inputs are finite; a program needn't handle non-finite values.
Results may differ from the reference program's by a relative error of at most 0.0011.
Values may be sent and summed in bfloat16 or wider, within the bound.
A program may use at most 64 MiB of HBM per device.

```python
import math
import jax
import jax.numpy as jnp
from jax import lax

LEAF = 1024
RANK = 256
COLS = 512
LPG = 4
NEAR = 3
GROUPS = 16
GROUP_ROWS = 4096


def draw_near_lists(key, part):
    group_keys = jax.random.split(jax.random.fold_in(key, 17), GROUPS)
    counting = jnp.arange(LPG, dtype=jnp.int32)

    def one_group(group_key):
        order = jax.random.permutation(group_key, LPG).astype(jnp.int32)
        place = jnp.zeros((LPG,), jnp.int32).at[order].set(counting)
        successor = order[(place + 1) % LPG]
        predecessor = order[(place + LPG - 1) % LPG]
        return jnp.stack([counting, successor, predecessor], axis=1)
    return jax.vmap(one_group)(group_keys).astype(jnp.int32)


def shard_levels(stream_key, dims, cuts, smallest, largest):
    def one(dim, parts):
        draws = jax.random.uniform(jax.random.fold_in(jax.random.fold_in(stream_key, 6), dim), (parts,), jnp.float32, smallest / len(cuts), largest / len(cuts))
        return jnp.repeat(jnp.exp(draws), dims[dim] // parts).reshape((-1,) + (1,) * (len(dims) - dim - 1))

    factor_of = one(*cuts[0])
    for cut in cuts[1:]:
        factor_of = factor_of * one(*cut)
    return factor_of


def noise(stream_key, dims, spread, reach, cuts=(), kind=jnp.bfloat16):
    array = jax.random.normal(stream_key, dims, jnp.float32) * spread
    if len(cuts) > 0:
        array = shard_levels(stream_key, dims, cuts, -0.22, 0.18) * array
    return jnp.clip(array, min=-reach, max=reach).astype(kind)


def setup_inputs(seed: int = 0) -> dict:
    splits = jax.random.split(jax.random.key(seed), 9)
    return {
        "coefficients": noise(splits[0], (GROUPS, GROUP_ROWS, COLS), 1.0, 6.0, ((0, 16), (1, 32)), jnp.float32),
        "labels": noise(splits[1], (GROUPS, GROUP_ROWS, COLS), 1.0, 6.0, ((0, 16), (1, 32)), jnp.float32),
        "near_kernel": noise(splits[2], (GROUPS, GROUP_ROWS, NEAR * LEAF), (NEAR * LEAF) ** -0.5, 0.109375, ((0, 16), (1, 32)), jnp.float32),
        "basis": noise(splits[3], (GROUPS, GROUP_ROWS, RANK), LEAF ** -0.5, 0.1875, ((0, 16), (1, 32)), jnp.float32),
        "transfer": noise(splits[4], (GROUPS, LPG * RANK, RANK), RANK ** -0.5, 0.375, ((0, 16), (1, 32)), jnp.float32),
        "coupling": noise(splits[5], (GROUPS, RANK, GROUPS * RANK), (GROUPS * RANK) ** -0.5, 0.09375, ((0, 16), (1, 32)), jnp.float32),
        "near_lists": draw_near_lists(jax.random.fold_in(splits[8], 71), 0),
        "ridge": jnp.clip(jnp.exp(jax.random.uniform(splits[7], (1,), jnp.float32, math.log(0.5), math.log(2.0))), 0.5, 2.0),
    }


def reference(coefficients, labels, near_kernel, basis, transfer, coupling, near_lists, ridge):
    highest = lax.Precision.HIGHEST
    groups = coefficients.shape[0]
    leaves = coefficients.reshape(groups, LPG, LEAF, COLS)
    group_index = jnp.arange(groups, dtype=jnp.int32)[:, None, None]
    nearby = leaves[group_index, near_lists]
    kernel_blocks = near_kernel.reshape(groups, LPG, LEAF, NEAR, LEAF)
    near = jnp.einsum("giasb,gisbc->giac", kernel_blocks, nearby, precision=highest)
    leaf_basis = basis.reshape(groups, LPG, LEAF, RANK)
    leaf_coef = jnp.einsum("giar,giac->girc", leaf_basis, leaves, precision=highest)
    transfers = transfer.reshape(groups, LPG, RANK, RANK)
    group_coef = jnp.einsum("girs,girc->gsc", transfers, leaf_coef, precision=highest)
    group_round = lax.optimization_barrier(group_coef.astype(jnp.bfloat16)).astype(jnp.float32)
    stacked = group_round.reshape(groups * RANK, COLS)
    coarse = jnp.einsum("gsk,kc->gsc", coupling, stacked, precision=highest)
    downward = jnp.einsum("girs,gsc->girc", transfers, coarse, precision=highest)
    far = jnp.einsum("giar,girc->giac", leaf_basis, downward, precision=highest)
    total = near + far + ridge[0] * leaves
    result = labels.reshape(groups, LPG, LEAF, COLS) - total
    return result.reshape(groups, LPG * LEAF, COLS)
```

```python
import functools

import jax
import jax.numpy as jnp
from jax import lax
from jax.experimental import pallas as pl
from jax.experimental.pallas import tpu as pltpu
from jax.sharding import PartitionSpec as P

F32 = jnp.float32
BF16 = jnp.bfloat16
I16 = jnp.int16
HIGHEST = lax.Precision.HIGHEST
MESH = pl.DeviceIdType.MESH

ROWS = 128
CODED = ROWS + 16
NEAR = 3
LINKS = 96


def dot(a, b, precision=None):
    return jnp.dot(a, b, precision=precision, preferred_element_type=F32)


def split(a):
    high = a.astype(BF16)
    return high, (a - high.astype(F32)).astype(BF16)


def encode(w):
    peak = jnp.maximum(jnp.max(jnp.abs(w), axis=0, keepdims=True), 1e-30)
    exponent = jnp.ceil(jnp.log2(peak) + 1e-3)
    codes = jnp.round(w * (jnp.exp2(-exponent) * 32767.0))
    codes = jnp.clip(codes, -32767.0, 32767.0).astype(jnp.int32).astype(I16)
    return codes, jnp.broadcast_to(exponent, (16, w.shape[1])).astype(jnp.int32).astype(I16)


def decode(coded):
    codes = coded[:ROWS].astype(jnp.int32).astype(F32)
    exponent = coded[ROWS:].astype(jnp.int32).astype(F32)[:1]
    return codes * (jnp.exp2(exponent) * (1.0 / 32767.0))


def kernel(
    coef, labels, near_kernel, basis, transfer, coupling, lists, ridge, out,
    kraw, khl, wz, wx, near, efull, bmat, cplb, chl, pown, pgive, pgot, hx, rs,
    s1, r1, s2, r2, stack, cgive, cgot, cb, ksem, ssem, rsem,
):
    me = lax.axis_index("leaf")
    g = lax.axis_index("group")
    zh = me // 8
    pos = lax.rem(me, 8)
    x = pos // 2
    c = lax.rem(pos, 2)
    oc = 1 - c
    up, down = lax.rem(zh + 1, 4), lax.rem(zh + 3, 4)
    right, left = lax.rem(x + 1, 4), lax.rem(x + 3, 4)
    beyond = lax.rem(x + 2, 4)
    partner = me + 1 - 2 * c

    def leaf_at(z_, x_, c_):
        return z_ * 8 + x_ * 2 + c_

    to_right, to_left = leaf_at(zh, right, c), leaf_at(zh, left, c)
    to_up, to_down = leaf_at(up, x, c), leaf_at(down, x, c)
    row_peers = [zh * 8 + lax.rem(pos + d, 8) for d in range(1, 8)]
    group_peers = [lax.rem(g + d, 16) for d in range(1, 16)]

    sent = []

    def send(src, dst, leaf=None, group=None):
        i = len(sent)
        target = {"leaf": leaf} if group is None else {"group": group}
        copy = pltpu.make_async_remote_copy(
            src_ref=src, dst_ref=dst, send_sem=ssem.at[i], recv_sem=rsem.at[i],
            device_id=target, device_id_type=MESH,
        )
        copy.start()
        sent.append(copy)
        return copy

    kcopy = pltpu.make_async_copy(near_kernel.at[0], kraw, ksem)
    kcopy.start()

    barrier = pltpu.get_barrier_semaphore()
    for peer in row_peers + [to_up, to_down]:
        pl.semaphore_signal(barrier, inc=1, device_id={"leaf": peer}, device_id_type=MESH)
    for peer in group_peers:
        pl.semaphore_signal(barrier, inc=1, device_id={"group": peer}, device_id_type=MESH)

    codes, exponents = encode(coef[0])
    wz[zh, :ROWS] = codes
    wz[zh, ROWS:] = exponents
    wx[0, x, c, :ROWS] = codes
    wx[0, x, c, ROWS:] = exponents
    cplb[x, c] = coupling[0]
    own_rows = pl.ds(pl.multiple_of(pos * 32, 32), 32)
    efull[own_rows, :] = transfer[0]
    pl.semaphore_wait(barrier, len(row_peers) + 2 + len(group_peers))

    e_in = [send(transfer.at[0], efull.at[own_rows, :], leaf=p) for p in row_peers]
    wz_up = send(wz.at[zh], wz.at[zh], leaf=to_up)
    wz_down = send(wz.at[zh], wz.at[zh], leaf=to_down)

    kcopy.wait()

    @pl.loop(0, 12)
    def _(b):
        high, low = split(kraw[:, pl.ds(pl.multiple_of(b * 256, 256), 256)])
        khl[b, :ROWS] = high
        khl[b, ROWS:] = low

    for copy in e_in:
        copy.wait_recv()
    bm = dot(basis[0], efull[...], HIGHEST)
    bmat[...] = bm
    part = lax.dot_general(
        bm, coef[0], (((0,), (0,)), ((), ())), precision=HIGHEST, preferred_element_type=F32
    )
    low_half, high_half = part[:ROWS], part[ROWS:]
    keep = jnp.where(c == 0, low_half, high_half)
    give = jnp.where(c == 0, high_half, low_half)
    for k in range(4):
        pown[k] = keep[:, k * 128:(k + 1) * 128]
        pgive[k] = give[:, k * 128:(k + 1) * 128]
    core_sum = send(pgive, pgot, leaf=partner)
    core_sum.wait_recv()
    hx[...] = pown[...] + pgot[...]
    rs_in = []
    for d in range(1, 4):
        xd = lax.rem(x + d, 4)
        rs_in.append(send(hx.at[xd], rs.at[d - 1], leaf=leaf_at(zh, xd, c)))

    def gather_start(piece):
        return [send(piece(x), piece(x), leaf=p) for p in (to_right, to_left, partner)]

    def gather_relay(copies, piece, first, second):
        copies[0].wait_recv()
        copies += [
            send(first(left), first(left), leaf=to_right),
            send(piece(left), piece(left), leaf=partner),
        ]
        copies[1].wait_recv()
        copies += [
            send(second(right), second(right), leaf=to_left),
            send(piece(right), piece(right), leaf=partner),
        ]

    def gather_end(copies, piece):
        copies[3].wait_recv()
        copies[5].wait_recv()
        copies.append(send(piece(beyond), piece(beyond), leaf=partner))

    def gather_wait(copies):
        for i in (2, 4, 6, 7):
            copies[i].wait_recv()

    def w_pieces(n):
        return (
            lambda k: wx.at[n, k, c],
            lambda k: wx.at[n, k, c, pl.ds(0, 64)],
            lambda k: wx.at[n, k, c, pl.ds(64, CODED - 64)],
        )

    cpl_pieces = (
        lambda k: cplb.at[k, c],
        lambda k: cplb.at[k, c, :, pl.ds(0, 2048)],
        lambda k: cplb.at[k, c, :, pl.ds(2048, 2048)],
    )

    cpl_g = gather_start(cpl_pieces[0])
    w0 = w_pieces(0)
    w0_g = gather_start(w0[0])

    for copy in rs_in:
        copy.wait_recv()
    s1[...] = (hx[x] + rs[0]) + (rs[1] + rs[2])
    near_z, other_z = leaf_at(zh + 1 - 2 * lax.rem(zh, 2), x, c), leaf_at(3 - zh, x, c)
    lo, hi = pl.ds(0, 64), pl.ds(64, 64)
    ar = [
        send(s1.at[lo], r1.at[lo], leaf=near_z),
        send(s1.at[hi], r1.at[hi], leaf=other_z),
    ]

    gather_relay(w0_g, *w0)
    gather_relay(cpl_g, *cpl_pieces)

    ar[0].wait_recv()
    ar[1].wait_recv()
    s2[...] = s1[...] + r1[...]
    ar += [
        send(s2.at[lo], r2.at[lo], leaf=other_z),
        send(s2.at[hi], r2.at[hi], leaf=near_z),
    ]

    first_rows, last_rows = pl.ds(0, 64), pl.ds(64, CODED - 64)
    wz_up.wait_recv()
    wz_far_up = send(wz.at[down, first_rows], wz.at[down, first_rows], leaf=to_up)
    wz_down.wait_recv()
    wz_far_down = send(wz.at[up, last_rows], wz.at[up, last_rows], leaf=to_down)

    gather_end(w0_g, w0[0])
    gather_end(cpl_g, cpl_pieces[0])

    ar[2].wait_recv()
    ar[3].wait_recv()
    stack[g] = (s2[...] + r2[...]).astype(BF16)
    st_in = [send(stack.at[g], stack.at[g], group=p) for p in group_peers]

    wz_far_up.wait_recv()
    wz_far_down.wait_recv()
    w_g = [w0_g]
    for n in range(1, NEAR):
        wx[n, x, c] = wz[lists[0, zh, n]]
        w_g.append(gather_start(w_pieces(n)[0]))

    def add_near(n):
        @pl.loop(0, 4)
        def _(k):
            b = n * 4 + k
            w = jnp.concatenate([decode(wx[n, k, 0]), decode(wx[n, k, 1])], axis=0)
            high, low = split(w)
            both = dot(khl[b], high)
            term = both[:ROWS] + both[ROWS:] + dot(khl[b, :ROWS], low)
            near[...] += term

    near[...] = jnp.zeros_like(near)
    gather_wait(w0_g)
    add_near(0)

    gather_wait(cpl_g)
    for h in range(16):
        cols = pl.ds(pl.multiple_of(h * 256 + c * 128, 128), 128)
        high, low = split(cplb[:, :, :, cols].reshape(64, 128))
        chl[:64, h * 128:(h + 1) * 128] = high
        chl[64:, h * 128:(h + 1) * 128] = low

    for n in range(1, NEAR):
        gather_relay(w_g[n], *w_pieces(n))

    for copy in st_in:
        copy.wait_recv()
    both = dot(chl[...], stack[...].reshape(2048, 128))
    block = both[:64] + both[64:]
    cgive[...] = jnp.where(c == 0, block[32:], block[:32])
    core_part = jnp.where(c == 0, block[:32], block[32:])
    core_sum2 = send(cgive, cgot, leaf=partner)
    core_sum2.wait_recv()
    cb[x, zh, c] = core_part + cgot[...]
    cz = [
        send(cb.at[x, zh, c], cb.at[x, zh, c], leaf=to_up),
        send(cb.at[x, zh, c], cb.at[x, zh, c], leaf=to_down),
    ]
    for n in range(1, NEAR):
        gather_end(w_g[n], w_pieces(n)[0])
    cz[0].wait_recv()
    cz.append(send(cb.at[x, down, c, pl.ds(0, 16)], cb.at[x, down, c, pl.ds(0, 16)], leaf=to_up))
    cz[1].wait_recv()
    cz.append(send(cb.at[x, up, c, pl.ds(16, 16)], cb.at[x, up, c, pl.ds(16, 16)], leaf=to_down))
    gather_wait(w_g[1])
    add_near(1)
    cz[2].wait_recv()
    cz[3].wait_recv()
    cb_pieces = (
        lambda k: cb.at[k, :, c],
        lambda k: cb.at[k, pl.ds(0, 2), c],
        lambda k: cb.at[k, pl.ds(2, 2), c],
    )
    cb_g = gather_start(cb_pieces[0])
    gather_wait(w_g[2])
    add_near(2)
    gather_relay(cb_g, *cb_pieces)
    gather_end(cb_g, cb_pieces[0])
    gather_wait(cb_g)

    for k in range(4):
        cols = slice(k * 128, (k + 1) * 128)
        far = dot(bmat[...], cb[k].reshape(256, 128), HIGHEST)
        out[0, :, cols] = labels[0, :, cols] - (near[:, cols] + far + ridge[0] * coef[0, :, cols])

    for copy in sent:
        copy.wait_send()


def shards(*operands):
    vmem = pl.BlockSpec(memory_space=pltpu.VMEM)
    smem = pl.BlockSpec(memory_space=pltpu.SMEM)
    v = pltpu.VMEM
    return pl.pallas_call(
        kernel,
        out_shape=jax.ShapeDtypeStruct((1, ROWS, 512), F32),
        in_specs=[vmem, vmem, pl.BlockSpec(memory_space=pl.ANY), vmem, vmem, vmem, smem, smem],
        out_specs=vmem,
        scratch_shapes=[
            v((ROWS, 3072), F32),
            v((12, 256, 256), BF16),
            v((4, CODED, 512), I16),
            v((NEAR, 4, 2, CODED, 512), I16),
            v((ROWS, 512), F32),
            v((256, 256), F32),
            v((ROWS, 256), F32),
            v((4, 2, 8, 4096), F32),
            v((128, 2048), BF16),
            v((4, 128, 128), F32),
            v((4, 128, 128), F32),
            v((4, 128, 128), F32),
            v((4, 128, 128), F32),
            v((3, 128, 128), F32),
            v((128, 128), F32),
            v((128, 128), F32),
            v((128, 128), F32),
            v((128, 128), F32),
            v((16, 128, 128), BF16),
            v((32, 128), F32),
            v((32, 128), F32),
            v((4, 4, 2, 32, 128), F32),
            pltpu.SemaphoreType.DMA,
            pltpu.SemaphoreType.DMA((LINKS,)),
            pltpu.SemaphoreType.DMA((LINKS,)),
        ],
        compiler_params=pltpu.CompilerParams(
            collective_id=0, has_side_effects=True, vmem_limit_bytes=40 * 1024 * 1024
        ),
    )(*operands)


def solution(mesh):
    split_rows = P("group", "leaf", None)
    placed = (split_rows,) * 6 + (P("group", None, None), P())
    return jax.shard_map(
        shards, mesh=mesh, in_specs=placed, out_specs=split_rows, check_vma=False
    )
```

```python
import jax
import jax.numpy as jnp
from jax import lax
from jax.experimental import pallas as pl
from jax.experimental.pallas import tpu as pltpu
from jax.sharding import PartitionSpec as P

F32 = jnp.float32
BF16 = jnp.bfloat16
I16 = jnp.int16
HIGHEST = lax.Precision.HIGHEST
MESH = pl.DeviceIdType.MESH

ROWS = 128
TOP = 6.0
NEAR = 3
LINKS = 128


def dot(a, b, precision=None, dims=((1,), (0,))):
    return lax.dot_general(a, b, (dims, ((), ())), precision=precision, preferred_element_type=F32)


def split(a):
    high = a.astype(BF16)
    return high, (a - high.astype(F32)).astype(BF16)


def encode(w):
    root = jnp.sqrt(jnp.sqrt(jnp.minimum(jnp.abs(w) * (1.0 / TOP), 1.0)))
    return jnp.round(jnp.where(w < 0, -32767.0, 32767.0) * root).astype(jnp.int32).astype(I16)


def decode(codes):
    root = codes.astype(jnp.int32).astype(F32) * (1.0 / 32767.0)
    square = root * root
    return jnp.where(root < 0, -TOP, TOP) * (square * square)


def kernel(
    coef_in, labels_in, near_kernel, basis_in, transfer, coupling, lists_in, ridge, out,
    coef, labels, basis, lists, kraw, khl, wn, wf, wx, near, efull, bmat, cplb, chl,
    pt, pgot, hx, rs, s1, r1, s2, r2, stack, cb, lsem, ssem, rsem,
):
    me = lax.axis_index("leaf")
    g = lax.axis_index("group")
    zh = me // 8
    pos = lax.rem(me, 8)
    x = pos // 2
    c = lax.rem(pos, 2)
    oc = 1 - c
    y = g // 4
    zl = lax.rem(g, 4)

    def turn(i, d):
        return lax.rem(i + d, 4)

    up, down, across = turn(zh, 1), turn(zh, 3), turn(zh, 2)
    right, left, beyond = turn(x, 1), turn(x, 3), turn(x, 2)

    def leaf_at(z_, x_, c_):
        return z_ * 8 + x_ * 2 + c_

    to_right, to_left = leaf_at(zh, right, c), leaf_at(zh, left, c)
    to_up, to_down = leaf_at(up, x, c), leaf_at(down, x, c)
    partner = leaf_at(zh, x, oc)
    row_peers = [zh * 8 + lax.rem(pos + d, 8) for d in range(1, 8)]
    run_peers = [y * 4 + turn(zl, d) for d in range(1, 4)]
    to_north, to_south = turn(y, 1) * 4 + zl, turn(y, 3) * 4 + zl

    sent = []

    def send(src, dst, leaf=None, group=None):
        i = len(sent)
        target = {"leaf": leaf} if group is None else {"group": group}
        copy = pltpu.make_async_remote_copy(
            src_ref=src, dst_ref=dst, send_sem=ssem.at[i], recv_sem=rsem.at[i],
            device_id=target, device_id_type=MESH,
        )
        copy.start()
        sent.append(copy)
        return copy

    def same(ref, leaf=None, group=None):
        return send(ref, ref, leaf, group)

    own_rows = pl.ds(pl.multiple_of(pos * 32, 32), 32)
    loads = [
        pltpu.make_async_copy(src, dst, lsem.at[i])
        for i, (src, dst) in enumerate([
            (coef_in.at[0], coef), (basis_in.at[0], basis), (transfer.at[0], efull.at[own_rows, :]),
            (coupling.at[0], cplb.at[x, c]), (near_kernel.at[0], kraw), (labels_in.at[0], labels),
            (lists_in, lists),
        ])
    ]
    for load in loads:
        load.start()

    barrier = pltpu.get_barrier_semaphore()
    for peer in row_peers + [to_up, to_down]:
        pl.semaphore_signal(barrier, inc=1, device_id={"leaf": peer}, device_id_type=MESH)
    for peer in run_peers + [to_north, to_south]:
        pl.semaphore_signal(barrier, inc=1, device_id={"group": peer}, device_id_type=MESH)

    loads[0].wait()
    loads[1].wait()
    part = dot(coef[...], basis[...], HIGHEST, ((0,), (0,)))
    for k in range(4):
        for h in range(2):
            pt[k, h] = part[(2 * k + h) * 64:(2 * k + h + 1) * 64]
    wx[0, x, c] = encode(coef[...])
    loads[2].wait()
    pl.semaphore_wait(barrier, len(row_peers) + len(run_peers) + 4)

    core_sum = send(pt.at[:, oc], pgot, leaf=partner)

    def gather_start(piece):
        return [same(piece(x), leaf=p) for p in (to_right, to_left, partner)]

    def gather_relay(copies, piece, first, second):
        copies[0].wait_recv()
        copies += [same(first(left), leaf=to_right), same(piece(left), leaf=partner)]
        copies[1].wait_recv()
        copies += [same(second(right), leaf=to_left), same(piece(right), leaf=partner)]

    def gather_end(copies, piece, *_):
        copies[3].wait_recv()
        copies[5].wait_recv()
        copies.append(same(piece(beyond), leaf=partner))

    def gather_wait(copies):
        for i in (2, 4, 6, 7):
            copies[i].wait_recv()

    def e_rows(k, start, size):
        return efull.at[pl.ds(pl.multiple_of((2 * k + c) * 32 + start, 16), size), :]

    e_pieces = (
        lambda k: e_rows(k, 0, 32), lambda k: e_rows(k, 0, 16), lambda k: e_rows(k, 16, 16)
    )
    cpl_pieces = (
        lambda k: cplb.at[k, c],
        lambda k: cplb.at[k, c, :, pl.ds(0, 2048)],
        lambda k: cplb.at[k, c, :, pl.ds(2048, 2048)],
    )

    def w_pieces(n):
        return (
            lambda k: wx.at[n, k, c],
            lambda k: wx.at[n, k, c, pl.ds(0, 64)],
            lambda k: wx.at[n, k, c, pl.ds(64, 64)],
        )

    e_g = gather_start(e_pieces[0])
    w_up = send(wx.at[0, x, c], wn.at[0], leaf=to_up)
    w_down = send(wx.at[0, x, c], wn.at[1], leaf=to_down)
    core_sum.wait_recv()
    hx[...] = pt[:, c] + pgot[...]
    rs_in = [
        send(hx.at[turn(x, d)], rs.at[d - 1], leaf=leaf_at(zh, turn(x, d), c)) for d in range(1, 4)
    ]
    gather_relay(e_g, *e_pieces)
    loads[3].wait()
    cpl_g = gather_start(cpl_pieces[0])
    w_g = [gather_start(w_pieces(0)[0])]
    gather_end(e_g, *e_pieces)
    gather_wait(e_g)

    for copy in rs_in:
        copy.wait_recv()
    group = dot((hx[x] + rs[0]) + (rs[1] + rs[2]), efull[...], HIGHEST).T
    s1[...] = jnp.concatenate([group[:128], group[128:]], axis=1)
    near_z, other_z = leaf_at(zh + 1 - 2 * lax.rem(zh, 2), x, c), leaf_at(3 - zh, x, c)
    lo, hi = pl.ds(0, 64), pl.ds(64, 64)
    ar = [
        send(s1.at[lo], r1.at[lo], leaf=near_z),
        send(s1.at[hi], r1.at[hi], leaf=other_z),
    ]
    bmat[...] = dot(basis[...], efull[...], HIGHEST)
    for load in loads[4:]:
        load.wait()

    @pl.loop(0, 12)
    def _(b):
        high, low = split(kraw[:, pl.ds(pl.multiple_of(b * 256, 256), 256)])
        khl[b, :ROWS] = high
        khl[b, ROWS:] = low

    gather_relay(cpl_g, *cpl_pieces)
    gather_relay(w_g[0], *w_pieces(0))
    ar[0].wait_recv()
    ar[1].wait_recv()
    s2[...] = s1[...] + r1[...]
    ar += [
        send(s2.at[lo], r2.at[lo], leaf=other_z),
        send(s2.at[hi], r2.at[hi], leaf=near_z),
    ]

    w_up.wait_recv()
    far_up = send(wn.at[0, pl.ds(0, 64)], wf.at[pl.ds(0, 64)], leaf=to_up)
    w_down.wait_recv()
    far_down = send(
        wn.at[1, pl.ds(64, 64)], wf.at[pl.ds(64, 64)], leaf=to_down
    )
    one, two = lists[1, 0, zh], lists[2, 0, zh]
    one_adjacent = lax.rem(one + zh, 2)
    adjacent = one_adjacent * one + (1 - one_adjacent) * two
    last = one + two - adjacent
    last_across = 1 - lax.rem(last + zh, 2)
    entry = [0, 2 - one_adjacent, 1 + one_adjacent]
    is_up = lax.rem(adjacent + 4 - zh, 4) == 1
    wx[1, x, c] = jnp.where(is_up, wn[1], wn[0])
    w_g.append(gather_start(w_pieces(1)[0]))
    gather_end(w_g[0], *w_pieces(0))
    gather_end(cpl_g, *cpl_pieces)

    ar[2].wait_recv()
    ar[3].wait_recv()
    stack[g] = (s2[...] + r2[...]).astype(BF16)
    runs = [same(stack.at[g], group=p) for p in run_peers]
    rings = [[same(stack.at[g], group=to_north), same(stack.at[g], group=to_south)]]
    for d in range(1, 4):
        runs[d - 1].wait_recv()
        ref = stack.at[y * 4 + turn(zl, 4 - d)]
        rings.append([same(ref, group=to_north), same(ref, group=to_south)])
    gather_relay(w_g[1], *w_pieces(1))
    for d in range(4):
        zd = turn(zl, 4 - d)
        rings[d][0].wait_recv()
        rings[d].append(same(stack.at[turn(y, 3) * 4 + zd, lo], group=to_north))
        rings[d][1].wait_recv()
        rings[d].append(same(stack.at[turn(y, 1) * 4 + zd, hi], group=to_south))

    far_up.wait_recv()
    far_down.wait_recv()
    other = jnp.where(is_up, wn[0], wn[1])
    wx[2, x, c] = jnp.where(last_across == 1, wf[...], other)
    w_g.append(gather_start(w_pieces(2)[0]))

    def add_near(n):
        @pl.loop(0, 4)
        def _(k):
            b = entry[n] * 4 + k
            w = jnp.concatenate([decode(wx[n, k, 0]), decode(wx[n, k, 1])], axis=0)
            high, low = split(w)
            block = khl[b]
            both = dot(block, high)
            near[...] -= both[:ROWS] + both[ROWS:] + dot(block[:ROWS], low)

    near[...] = labels[...] - ridge[0] * coef[...]
    gather_wait(cpl_g)
    for h in range(16):
        for half in range(2):
            start = h * 256 + half * 128
            high, low = split(cplb[:, :, :, start:start + 128].reshape(64, 128))
            chl[half * 128:half * 128 + 64, h * 128:(h + 1) * 128] = high
            chl[half * 128 + 64:(half + 1) * 128, h * 128:(h + 1) * 128] = low
    gather_wait(w_g[0])
    add_near(0)
    gather_end(w_g[1], *w_pieces(1))

    for ring in rings:
        ring[2].wait_recv()
        ring[3].wait_recv()
    both = dot(chl[...], stack[...].reshape(2048, 128))
    first, second = both[:64] + both[64:128], both[128:192] + both[192:]
    block = first[:, :64] + second[:, 64:]
    cb[zh, pos] = jnp.concatenate([block[:32], block[32:]], axis=1)

    def to_row(z_):
        return [same(cb.at[z_, pos], leaf=p) for p in row_peers]

    cz = [same(cb.at[zh, pos], leaf=p) for p in (to_up, to_down)]
    cb_in = to_row(zh)
    gather_relay(w_g[2], *w_pieces(2))
    cz[0].wait_recv()
    cz.append(same(cb.at[down, pos, pl.ds(0, 16)], leaf=to_up))
    cb_in += to_row(down)
    cz[1].wait_recv()
    cz.append(same(cb.at[up, pos, pl.ds(16, 16)], leaf=to_down))
    cb_in += to_row(up)
    gather_wait(w_g[1])
    add_near(1)
    cz[2].wait_recv()
    cz[3].wait_recv()
    cb_in += to_row(across)
    gather_end(w_g[2], *w_pieces(2))
    gather_wait(w_g[2])
    add_near(2)
    for copy in cb_in:
        copy.wait_recv()

    for k in range(4):
        rows = []
        for z_ in range(4):
            a, b = cb[z_, 2 * k], cb[z_, 2 * k + 1]
            rows += [
                jnp.concatenate([a[:, :64], b[:, :64]], axis=1),
                jnp.concatenate([a[:, 64:], b[:, 64:]], axis=1),
            ]
        cols = slice(k * 128, (k + 1) * 128)
        far = dot(bmat[...], jnp.concatenate(rows, axis=0), HIGHEST)
        out[0, :, cols] = near[:, cols] - far

    for copy in sent:
        copy.wait_send()


def shards(coef, labels, near_kernel, basis, transfer, coupling, lists, ridge):
    operands = coef, labels, near_kernel, basis, transfer, coupling, lists.transpose(2, 0, 1), ridge
    v = pltpu.VMEM
    hbm = pl.BlockSpec(memory_space=pltpu.HBM)
    return pl.pallas_call(
        kernel,
        out_shape=jax.ShapeDtypeStruct((1, ROWS, 512), F32),
        in_specs=[hbm] * 7 + [pl.BlockSpec(memory_space=pltpu.SMEM)],
        out_specs=pl.BlockSpec(memory_space=v),
        scratch_shapes=[
            v((ROWS, 512), F32),
            v((ROWS, 512), F32),
            v((ROWS, 256), F32),
            pltpu.SMEM((NEAR, 1, 4), jnp.int32),
            v((ROWS, 3072), F32),
            v((12, 256, 256), BF16),
            v((2, ROWS, 512), I16),
            v((ROWS, 512), I16),
            v((NEAR, 4, 2, ROWS, 512), I16),
            v((ROWS, 512), F32),
            v((256, 256), F32),
            v((ROWS, 256), F32),
            v((4, 2, 8, 4096), F32),
            v((256, 2048), BF16),
            v((4, 2, 64, 256), F32),
            v((4, 64, 256), F32),
            v((4, 64, 256), F32),
            v((3, 64, 256), F32),
            v((128, 128), F32),
            v((128, 128), F32),
            v((128, 128), F32),
            v((128, 128), F32),
            v((16, 128, 128), BF16),
            v((4, 8, 32, 128), F32),
            pltpu.SemaphoreType.DMA((7,)),
            pltpu.SemaphoreType.DMA((LINKS,)),
            pltpu.SemaphoreType.DMA((LINKS,)),
        ],
        compiler_params=pltpu.CompilerParams(
            collective_id=0, has_side_effects=True, vmem_limit_bytes=67_043_328
        ),
    )(*operands)


def solution(mesh):
    split_rows = P("group", "leaf", None)
    placed = (split_rows,) * 6 + (P("group", None, None), P())
    return jax.shard_map(
        shards, mesh=mesh, in_specs=placed, out_specs=split_rows, check_vma=False
    )
```

```python
import jax
import jax.numpy as jnp
from jax import lax
from jax.experimental import pallas as pl
from jax.experimental.pallas import tpu as pltpu
from jax.sharding import PartitionSpec as P

F32 = jnp.float32
BF16 = jnp.bfloat16
I16 = jnp.int16
HIGHEST = lax.Precision.HIGHEST
MESH = pl.DeviceIdType.MESH

ROWS = 128
TOP = 6.0
NEAR = 3
LINKS = 128


def dot(a, b, precision=None, dims=((1,), (0,))):
    return lax.dot_general(a, b, (dims, ((), ())), precision=precision, preferred_element_type=F32)


def split(a):
    high = a.astype(BF16)
    return high, (a - high.astype(F32)).astype(BF16)


def encode(w):
    root = jnp.sqrt(jnp.sqrt(jnp.minimum(jnp.abs(w) * (1.0 / TOP), 1.0)))
    return jnp.round(jnp.where(w < 0, -32767.0, 32767.0) * root).astype(jnp.int32).astype(I16)


def decode(codes):
    root = codes.astype(jnp.int32).astype(F32) * (1.0 / 32767.0)
    square = root * root
    return jnp.where(root < 0, -TOP, TOP) * (square * square)


def pack(v):
    peak = jnp.maximum(jnp.max(jnp.abs(v), axis=0, keepdims=True), 1e-30)
    exponent = jnp.ceil(jnp.log2(peak) + 1e-3)
    codes = jnp.clip(jnp.round(v * (jnp.exp2(-exponent) * 32767.0)), -32767.0, 32767.0)
    both = jnp.concatenate([codes, jnp.broadcast_to(exponent, (16, v.shape[1]))], axis=0)
    return both.astype(jnp.int32).astype(I16)


def unpack(coded):
    v = coded.astype(jnp.int32).astype(F32)
    return v[:-16] * (jnp.exp2(v[-16:-15]) * (1.0 / 32767.0))


def kernel(
    coef_in, labels_in, near_kernel, basis_in, transfer, coupling, lists_in, ridge, out,
    coef, labels, basis, lists, kraw, khl, wn, wf, wx, near, efull, bmat, cplb, chl,
    pt, pgot, hx, hc, rs, c1, r1, c2, r2, stack, cb, lsem, ssem, rsem,
):
    me = lax.axis_index("leaf")
    g = lax.axis_index("group")
    zh = me // 8
    pos = lax.rem(me, 8)
    x = pos // 2
    c = lax.rem(pos, 2)
    oc = 1 - c
    y = g // 4
    zl = lax.rem(g, 4)

    def turn(i, d):
        return lax.rem(i + d, 4)

    up, down, across = turn(zh, 1), turn(zh, 3), turn(zh, 2)
    right, left, beyond = turn(x, 1), turn(x, 3), turn(x, 2)

    def leaf_at(z_, x_, c_):
        return z_ * 8 + x_ * 2 + c_

    to_right, to_left = leaf_at(zh, right, c), leaf_at(zh, left, c)
    to_up, to_down = leaf_at(up, x, c), leaf_at(down, x, c)
    partner = leaf_at(zh, x, oc)
    row_peers = [zh * 8 + lax.rem(pos + d, 8) for d in range(1, 8)]
    run_peers = [y * 4 + turn(zl, d) for d in range(1, 4)]
    to_north, to_south = turn(y, 1) * 4 + zl, turn(y, 3) * 4 + zl

    sent = []

    def send(src, dst, leaf=None, group=None):
        i = len(sent)
        target = {"leaf": leaf} if group is None else {"group": group}
        copy = pltpu.make_async_remote_copy(
            src_ref=src, dst_ref=dst, send_sem=ssem.at[i], recv_sem=rsem.at[i],
            device_id=target, device_id_type=MESH,
        )
        copy.start()
        sent.append(copy)
        return copy

    def same(ref, leaf=None, group=None):
        return send(ref, ref, leaf, group)

    own_rows = pl.ds(pl.multiple_of(pos * 32, 32), 32)
    loads = [
        pltpu.make_async_copy(src, dst, lsem.at[i])
        for i, (src, dst) in enumerate([
            (coef_in.at[0], coef), (basis_in.at[0], basis), (transfer.at[0], efull.at[own_rows, :]),
            (coupling.at[0], cplb.at[x, c]), (near_kernel.at[0], kraw), (labels_in.at[0], labels),
            (lists_in, lists),
        ])
    ]
    for load in loads:
        load.start()

    barrier = pltpu.get_barrier_semaphore()
    for peer in row_peers + [to_up, to_down]:
        pl.semaphore_signal(barrier, inc=1, device_id={"leaf": peer}, device_id_type=MESH)
    for peer in run_peers + [to_north, to_south]:
        pl.semaphore_signal(barrier, inc=1, device_id={"group": peer}, device_id_type=MESH)

    loads[0].wait()
    loads[1].wait()
    part = dot(coef[...], basis[...], HIGHEST, ((0,), (0,)))
    for k in range(4):
        for h in range(2):
            pt[k, h] = part[(2 * k + h) * 64:(2 * k + h + 1) * 64]
    wx[0, x, c] = encode(coef[...])
    loads[2].wait()
    pl.semaphore_wait(barrier, len(row_peers) + len(run_peers) + 4)

    core_sum = send(pt.at[:, oc], pgot, leaf=partner)

    def gather_start(piece):
        return [same(piece(x), leaf=p) for p in (to_right, to_left, partner)]

    def gather_relay(copies, piece, first, second):
        copies[0].wait_recv()
        copies += [same(first(left), leaf=to_right), same(piece(left), leaf=partner)]
        copies[1].wait_recv()
        copies += [same(second(right), leaf=to_left), same(piece(right), leaf=partner)]

    def gather_end(copies, piece, *_):
        copies[3].wait_recv()
        copies[5].wait_recv()
        copies.append(same(piece(beyond), leaf=partner))

    def gather_wait(copies):
        for i in (2, 4, 6, 7):
            copies[i].wait_recv()

    def e_rows(k, start, size):
        return efull.at[pl.ds(pl.multiple_of((2 * k + c) * 32 + start, 16), size), :]

    e_pieces = (
        lambda k: e_rows(k, 0, 32), lambda k: e_rows(k, 0, 16), lambda k: e_rows(k, 16, 16)
    )
    cpl_pieces = (
        lambda k: cplb.at[k, c],
        lambda k: cplb.at[k, c, :, pl.ds(0, 2048)],
        lambda k: cplb.at[k, c, :, pl.ds(2048, 2048)],
    )

    def w_pieces(n):
        return (
            lambda k: wx.at[n, k, c],
            lambda k: wx.at[n, k, c, pl.ds(0, 64)],
            lambda k: wx.at[n, k, c, pl.ds(64, 64)],
        )

    e_g = gather_start(e_pieces[0])
    w_in = [
        send(wx.at[0, x, c, pl.ds(0, 64)], wn.at[0, pl.ds(0, 64)], leaf=to_up),
        send(wx.at[0, x, c, pl.ds(0, 64)], wn.at[1, pl.ds(0, 64)], leaf=to_down),
    ]
    core_sum.wait_recv()
    for k in range(4):
        both = pt[k, c] + pgot[k]
        hx[k] = jnp.concatenate([both[:, :128], both[:, 128:]], axis=0)
        hc[k] = pack(hx[k])
    rs_in = [
        send(hc.at[turn(x, d)], rs.at[d - 1], leaf=leaf_at(zh, turn(x, d), c)) for d in range(1, 4)
    ]
    gather_relay(e_g, *e_pieces)
    loads[3].wait()
    cpl_g = gather_start(cpl_pieces[0])
    w_g = [gather_start(w_pieces(0)[0])]
    gather_end(e_g, *e_pieces)
    gather_wait(e_g)

    for copy in rs_in:
        copy.wait_recv()
    total = (hx[x] + unpack(rs[0])) + (unpack(rs[1]) + unpack(rs[2]))
    total = jnp.concatenate([total[:64], total[64:]], axis=1)
    group = dot(total, efull[...], HIGHEST).T
    group = jnp.concatenate([group[:128], group[128:]], axis=1)
    c1[0], c1[1] = pack(group[:64]), pack(group[64:])
    near_z, other_z = leaf_at(zh + 1 - 2 * lax.rem(zh, 2), x, c), leaf_at(3 - zh, x, c)
    lo, hi = pl.ds(0, 64), pl.ds(64, 64)
    ar = [
        send(c1.at[0], r1.at[0], leaf=near_z),
        send(c1.at[1], r1.at[1], leaf=other_z),
    ]
    w_in += [
        send(wx.at[0, x, c, pl.ds(64, 64)], wn.at[0, pl.ds(64, 64)], leaf=to_up),
        send(wx.at[0, x, c, pl.ds(64, 64)], wn.at[1, pl.ds(64, 64)], leaf=to_down),
    ]
    bmat[...] = dot(basis[...], efull[...], HIGHEST)
    for load in loads[4:]:
        load.wait()

    @pl.loop(0, 12)
    def _(b):
        high, low = split(kraw[:, pl.ds(pl.multiple_of(b * 256, 256), 256)])
        khl[b, :ROWS] = high
        khl[b, ROWS:] = low

    gather_relay(cpl_g, *cpl_pieces)
    gather_relay(w_g[0], *w_pieces(0))
    ar[0].wait_recv()
    ar[1].wait_recv()
    for h in range(2):
        c2[h] = pack(unpack(c1[h]) + unpack(r1[h]))
    ar += [
        send(c2.at[0], r2.at[0], leaf=other_z),
        send(c2.at[1], r2.at[1], leaf=near_z),
    ]

    for copy in w_in:
        copy.wait_recv()
    one, two = lists[1, 0, zh], lists[2, 0, zh]
    one_adjacent = lax.rem(one + zh, 2)
    adjacent = one_adjacent * one + (1 - one_adjacent) * two
    last = one + two - adjacent
    last_across = 1 - lax.rem(last + zh, 2)
    entry = [0, 2 - one_adjacent, 1 + one_adjacent]
    is_up = lax.rem(adjacent + 4 - zh, 4) == 1
    wx[1, x, c] = jnp.where(is_up, wn[1], wn[0])
    w_g.append(gather_start(w_pieces(1)[0]))
    gather_end(w_g[0], *w_pieces(0))
    gather_end(cpl_g, *cpl_pieces)

    ar[2].wait_recv()
    ar[3].wait_recv()
    for h in range(2):
        stack[g, 64 * h:64 * (h + 1)] = (unpack(c2[h]) + unpack(r2[h])).astype(BF16)
    runs = [same(stack.at[g], group=p) for p in run_peers]
    rings = [[same(stack.at[g], group=to_north), same(stack.at[g], group=to_south)]]
    for d in range(1, 4):
        runs[d - 1].wait_recv()
        ref = stack.at[y * 4 + turn(zl, 4 - d)]
        rings.append([same(ref, group=to_north), same(ref, group=to_south)])
    far_up = send(wn.at[0, pl.ds(0, 64)], wf.at[pl.ds(0, 64)], leaf=to_up)
    far_down = send(
        wn.at[1, pl.ds(64, 64)], wf.at[pl.ds(64, 64)], leaf=to_down
    )
    gather_relay(w_g[1], *w_pieces(1))
    for d in range(4):
        zd = turn(zl, 4 - d)
        rings[d][0].wait_recv()
        rings[d].append(same(stack.at[turn(y, 3) * 4 + zd, lo], group=to_north))
        rings[d][1].wait_recv()
        rings[d].append(same(stack.at[turn(y, 1) * 4 + zd, hi], group=to_south))

    far_up.wait_recv()
    far_down.wait_recv()
    other = jnp.where(is_up, wn[0], wn[1])
    wx[2, x, c] = jnp.where(last_across == 1, wf[...], other)
    w_g.append(gather_start(w_pieces(2)[0]))

    def add_near(n):
        @pl.loop(0, 4)
        def _(k):
            b = entry[n] * 4 + k
            w = jnp.concatenate([decode(wx[n, k, 0]), decode(wx[n, k, 1])], axis=0)
            high, low = split(w)
            block = khl[b]
            both = dot(block, high)
            near[...] -= both[:ROWS] + both[ROWS:] + dot(block[:ROWS], low)

    near[...] = labels[...] - ridge[0] * coef[...]
    gather_wait(cpl_g)
    for h in range(16):
        for half in range(2):
            start = h * 256 + half * 128
            high, low = split(cplb[:, :, :, start:start + 128].reshape(64, 128))
            chl[half * 128:half * 128 + 64, h * 128:(h + 1) * 128] = high
            chl[half * 128 + 64:(half + 1) * 128, h * 128:(h + 1) * 128] = low
    gather_wait(w_g[0])
    add_near(0)
    gather_end(w_g[1], *w_pieces(1))

    for ring in rings:
        ring[2].wait_recv()
        ring[3].wait_recv()
    both = dot(chl[...], stack[...].reshape(2048, 128))
    first, second = both[:64] + both[64:128], both[128:192] + both[192:]
    block = first[:, :64] + second[:, 64:]
    cb[zh, pos] = jnp.concatenate([block[:32], block[32:]], axis=1)

    def to_row(z_):
        return [same(cb.at[z_, pos], leaf=p) for p in row_peers]

    cz = [same(cb.at[zh, pos], leaf=p) for p in (to_up, to_down, leaf_at(across, x, c))]
    cb_in = to_row(zh)
    gather_relay(w_g[2], *w_pieces(2))
    cz[0].wait_recv()
    cb_in += to_row(down)
    cz[1].wait_recv()
    cb_in += to_row(up)
    gather_wait(w_g[1])
    add_near(1)
    cz[2].wait_recv()
    cb_in += to_row(across)
    gather_end(w_g[2], *w_pieces(2))
    gather_wait(w_g[2])
    add_near(2)
    for copy in cb_in:
        copy.wait_recv()

    for k in range(4):
        rows = []
        for z_ in range(4):
            a, b = cb[z_, 2 * k], cb[z_, 2 * k + 1]
            rows += [
                jnp.concatenate([a[:, :64], b[:, :64]], axis=1),
                jnp.concatenate([a[:, 64:], b[:, 64:]], axis=1),
            ]
        cols = slice(k * 128, (k + 1) * 128)
        far = dot(bmat[...], jnp.concatenate(rows, axis=0), HIGHEST)
        out[0, :, cols] = near[:, cols] - far

    for copy in sent:
        copy.wait_send()


def shards(coef, labels, near_kernel, basis, transfer, coupling, lists, ridge):
    operands = coef, labels, near_kernel, basis, transfer, coupling, lists.transpose(2, 0, 1), ridge
    v = pltpu.VMEM
    hbm = pl.BlockSpec(memory_space=pltpu.HBM)
    return pl.pallas_call(
        kernel,
        out_shape=jax.ShapeDtypeStruct((1, ROWS, 512), F32),
        in_specs=[hbm] * 7 + [pl.BlockSpec(memory_space=pltpu.SMEM)],
        out_specs=pl.BlockSpec(memory_space=v),
        scratch_shapes=[
            v((ROWS, 512), F32),
            v((ROWS, 512), F32),
            v((ROWS, 256), F32),
            pltpu.SMEM((NEAR, 1, 4), jnp.int32),
            v((ROWS, 3072), F32),
            v((12, 256, 256), BF16),
            v((2, ROWS, 512), I16),
            v((ROWS, 512), I16),
            v((NEAR, 4, 2, ROWS, 512), I16),
            v((ROWS, 512), F32),
            v((256, 256), F32),
            v((ROWS, 256), F32),
            v((4, 2, 8, 4096), F32),
            v((256, 2048), BF16),
            v((4, 2, 64, 256), F32),
            v((4, 64, 256), F32),
            v((4, 128, 128), F32),
            v((4, 144, 128), I16),
            v((3, 144, 128), I16),
            v((2, 80, 128), I16),
            v((2, 80, 128), I16),
            v((2, 80, 128), I16),
            v((2, 80, 128), I16),
            v((16, 128, 128), BF16),
            v((4, 8, 32, 128), F32),
            pltpu.SemaphoreType.DMA((7,)),
            pltpu.SemaphoreType.DMA((LINKS,)),
            pltpu.SemaphoreType.DMA((LINKS,)),
        ],
        compiler_params=pltpu.CompilerParams(
            collective_id=0, has_side_effects=True, vmem_limit_bytes=67_043_328
        ),
    )(*operands)


def solution(mesh):
    split_rows = P("group", "leaf", None)
    placed = (split_rows,) * 6 + (P("group", None, None), P())
    return jax.shard_map(
        shards, mesh=mesh, in_specs=placed, out_specs=split_rows, check_vma=False
    )
```

```python
import jax
import jax.numpy as jnp
from jax import lax
from jax.experimental import pallas as pl
from jax.experimental.pallas import tpu as pltpu
from jax.sharding import PartitionSpec as P

F32 = jnp.float32
BF16 = jnp.bfloat16
I16 = jnp.int16
HIGHEST = lax.Precision.HIGHEST
MESH = pl.DeviceIdType.MESH

ROWS = 128
TOP = 6.0
NEAR = 3
LINKS = 128


def dot(a, b, precision=None, dims=((1,), (0,))):
    return lax.dot_general(a, b, (dims, ((), ())), precision=precision, preferred_element_type=F32)


def split(a):
    high = a.astype(BF16)
    return high, (a - high.astype(F32)).astype(BF16)


def encode(w):
    root = jnp.sqrt(jnp.sqrt(jnp.minimum(jnp.abs(w) * (1.0 / TOP), 1.0)))
    return jnp.round(jnp.where(w < 0, -32767.0, 32767.0) * root).astype(jnp.int32).astype(I16)


def decode(codes):
    root = codes.astype(jnp.int32).astype(F32) * (1.0 / 32767.0)
    square = root * root
    return jnp.where(root < 0, -TOP, TOP) * (square * square)


def pack(v):
    peak = jnp.maximum(jnp.max(jnp.abs(v), axis=0, keepdims=True), 1e-30)
    exponent = jnp.ceil(jnp.log2(peak) + 1e-3)
    codes = jnp.clip(jnp.round(v * (jnp.exp2(-exponent) * 32767.0)), -32767.0, 32767.0)
    both = jnp.concatenate([codes, jnp.broadcast_to(exponent, (16, v.shape[1]))], axis=0)
    return both.astype(jnp.int32).astype(I16)


def unpack(coded):
    v = coded.astype(jnp.int32).astype(F32)
    return v[:-16] * (jnp.exp2(v[-16:-15]) * (1.0 / 32767.0))


def kernel(
    coef_in, labels_in, near_kernel, basis_in, transfer, coupling, lists_in, ridge, out,
    coef, labels, basis, lists, kraw, khl, wn, wf, wx, near, efull, bmat, cplb, chl,
    pt, pgot, hx, hc, rs, c1, r1, c2, r2, stack, cb, lsem, ssem, rsem,
):
    me = lax.axis_index("leaf")
    g = lax.axis_index("group")
    zh = me // 8
    pos = lax.rem(me, 8)
    x = pos // 2
    c = lax.rem(pos, 2)
    oc = 1 - c
    y = g // 4
    zl = lax.rem(g, 4)

    def turn(i, d):
        return lax.rem(i + d, 4)

    up, down, across = turn(zh, 1), turn(zh, 3), turn(zh, 2)
    right, left, beyond = turn(x, 1), turn(x, 3), turn(x, 2)

    def leaf_at(z_, x_, c_):
        return z_ * 8 + x_ * 2 + c_

    to_right, to_left = leaf_at(zh, right, c), leaf_at(zh, left, c)
    to_up, to_down = leaf_at(up, x, c), leaf_at(down, x, c)
    partner = leaf_at(zh, x, oc)
    row_peers = [zh * 8 + lax.rem(pos + d, 8) for d in (4, 3, 5, 2, 6, 1, 7)]
    run_peers = [y * 4 + turn(zl, d) for d in range(1, 4)]
    to_north, to_south = turn(y, 1) * 4 + zl, turn(y, 3) * 4 + zl

    sent = []

    def send(src, dst, leaf=None, group=None):
        i = len(sent)
        target = {"leaf": leaf} if group is None else {"group": group}
        copy = pltpu.make_async_remote_copy(
            src_ref=src, dst_ref=dst, send_sem=ssem.at[i], recv_sem=rsem.at[i],
            device_id=target, device_id_type=MESH,
        )
        copy.start()
        sent.append(copy)
        return copy

    def same(ref, leaf=None, group=None):
        return send(ref, ref, leaf, group)

    own_rows = pl.ds(pl.multiple_of(pos * 32, 32), 32)
    loads = [
        pltpu.make_async_copy(src, dst, lsem.at[i])
        for i, (src, dst) in enumerate([
            (coef_in.at[0], coef), (basis_in.at[0], basis), (transfer.at[0], efull.at[own_rows, :]),
            (coupling.at[0], cplb.at[x, c]), (near_kernel.at[0], kraw), (labels_in.at[0], labels),
            (lists_in, lists),
        ])
    ]
    for load in loads:
        load.start()

    barrier = pltpu.get_barrier_semaphore()
    for peer in row_peers + [to_up, to_down]:
        pl.semaphore_signal(barrier, inc=1, device_id={"leaf": peer}, device_id_type=MESH)
    for peer in run_peers + [to_north, to_south]:
        pl.semaphore_signal(barrier, inc=1, device_id={"group": peer}, device_id_type=MESH)

    loads[0].wait()
    loads[1].wait()
    part = dot(coef[...], basis[...], HIGHEST, ((0,), (0,)))
    for k in range(4):
        for h in range(2):
            pt[k, h] = part[(2 * k + h) * 64:(2 * k + h + 1) * 64]
    wx[0, x, c] = encode(coef[...])
    loads[2].wait()
    pl.semaphore_wait(barrier, len(row_peers) + len(run_peers) + 4)

    core_sum = send(pt.at[:, oc], pgot, leaf=partner)

    def gather_start(piece):
        return [same(piece(x), leaf=p) for p in (to_right, to_left, partner)]

    def gather_relay(copies, piece, first, second):
        copies[0].wait_recv()
        copies += [same(first(left), leaf=to_right), same(piece(left), leaf=partner)]
        copies[1].wait_recv()
        copies += [same(second(right), leaf=to_left), same(piece(right), leaf=partner)]

    def gather_end(copies, piece, *_):
        copies[3].wait_recv()
        copies[5].wait_recv()
        copies.append(same(piece(beyond), leaf=partner))

    def gather_wait(copies):
        for i in (2, 4, 6, 7):
            copies[i].wait_recv()

    def e_rows(k, start, size):
        return efull.at[pl.ds(pl.multiple_of((2 * k + c) * 32 + start, 16), size), :]

    e_pieces = (
        lambda k: e_rows(k, 0, 32), lambda k: e_rows(k, 0, 16), lambda k: e_rows(k, 16, 16)
    )
    cpl_pieces = (
        lambda k: cplb.at[k, c],
        lambda k: cplb.at[k, c, :, pl.ds(0, 2048)],
        lambda k: cplb.at[k, c, :, pl.ds(2048, 2048)],
    )

    def w_pieces(n):
        return (
            lambda k: wx.at[n, k, c],
            lambda k: wx.at[n, k, c, pl.ds(0, 64)],
            lambda k: wx.at[n, k, c, pl.ds(64, 64)],
        )

    e_g = gather_start(e_pieces[0])
    w_in = [
        send(wx.at[0, x, c, pl.ds(0, 64)], wn.at[0, pl.ds(0, 64)], leaf=to_up),
        send(wx.at[0, x, c, pl.ds(0, 64)], wn.at[1, pl.ds(0, 64)], leaf=to_down),
    ]
    core_sum.wait_recv()
    for k in range(4):
        both = pt[k, c] + pgot[k]
        hx[k] = jnp.concatenate([both[:, :128], both[:, 128:]], axis=0)
        hc[k] = pack(hx[k])
    rs_in = [
        send(hc.at[turn(x, d)], rs.at[d - 1], leaf=leaf_at(zh, turn(x, d), c)) for d in range(1, 4)
    ]
    gather_relay(e_g, *e_pieces)
    loads[3].wait()
    cpl_g = gather_start(cpl_pieces[0])
    w_g = [gather_start(w_pieces(0)[0])]
    gather_end(e_g, *e_pieces)
    gather_wait(e_g)

    for copy in rs_in:
        copy.wait_recv()
    total = (hx[x] + unpack(rs[0])) + (unpack(rs[1]) + unpack(rs[2]))
    total = jnp.concatenate([total[:64], total[64:]], axis=1)
    group = dot(total, efull[...], HIGHEST).T
    group = jnp.concatenate([group[:128], group[128:]], axis=1)
    c1[0], c1[1] = pack(group[:64]), pack(group[64:])
    near_z, other_z = leaf_at(zh + 1 - 2 * lax.rem(zh, 2), x, c), leaf_at(3 - zh, x, c)
    lo, hi = pl.ds(0, 64), pl.ds(64, 64)
    ar = [
        send(c1.at[0], r1.at[0], leaf=near_z),
        send(c1.at[1], r1.at[1], leaf=other_z),
    ]
    w_in += [
        send(wx.at[0, x, c, pl.ds(64, 32)], wn.at[0, pl.ds(64, 32)], leaf=to_up),
        send(wx.at[0, x, c, pl.ds(64, 32)], wn.at[1, pl.ds(64, 32)], leaf=to_down),
    ]
    bmat[...] = dot(basis[...], efull[...], HIGHEST)
    for load in loads[4:]:
        load.wait()

    @pl.loop(0, 12)
    def _(b):
        high, low = split(kraw[:, pl.ds(pl.multiple_of(b * 256, 256), 256)])
        khl[b, :ROWS] = high
        khl[b, ROWS:] = low

    gather_relay(cpl_g, *cpl_pieces)
    gather_relay(w_g[0], *w_pieces(0))
    ar[0].wait_recv()
    ar[1].wait_recv()
    for h in range(2):
        c2[h] = pack(unpack(c1[h]) + unpack(r1[h]))
    ar += [
        send(c2.at[0], r2.at[0], leaf=other_z),
        send(c2.at[1], r2.at[1], leaf=near_z),
    ]

    def far_relay(start):
        first, second = pl.ds(start, 32), pl.ds(start + 32, 32)
        return [
            send(wn.at[0, first], wf.at[first], leaf=to_up),
            send(wn.at[1, second], wf.at[second], leaf=to_down),
        ]

    w_in += [
        send(wx.at[0, x, c, pl.ds(96, 32)], wn.at[0, pl.ds(96, 32)], leaf=to_up),
        send(wx.at[0, x, c, pl.ds(96, 32)], wn.at[1, pl.ds(96, 32)], leaf=to_down),
    ]
    for copy in w_in[:2]:
        copy.wait_recv()
    one, two = lists[1, 0, zh], lists[2, 0, zh]
    one_adjacent = lax.rem(one + zh, 2)
    adjacent = one_adjacent * one + (1 - one_adjacent) * two
    last = one + two - adjacent
    last_across = 1 - lax.rem(last + zh, 2)
    entry = [0, 2 - one_adjacent, 1 + one_adjacent]
    is_up = lax.rem(adjacent + 4 - zh, 4) == 1
    gather_end(w_g[0], *w_pieces(0))
    gather_end(cpl_g, *cpl_pieces)

    ar[2].wait_recv()
    ar[3].wait_recv()
    for h in range(2):
        stack[g, 64 * h:64 * (h + 1)] = (unpack(c2[h]) + unpack(r2[h])).astype(BF16)
    runs = [same(stack.at[g], group=p) for p in run_peers]
    rings = [[same(stack.at[g], group=to_north), same(stack.at[g], group=to_south)]]
    for copy in w_in[2:]:
        copy.wait_recv()
    wx[1, x, c] = jnp.where(is_up, wn[1], wn[0])
    w_g.append(gather_start(w_pieces(1)[0]))
    for d in range(1, 4):
        runs[d - 1].wait_recv()
        ref = stack.at[y * 4 + turn(zl, 4 - d)]
        rings.append([same(ref, group=to_north), same(ref, group=to_south)])
    far_in = [far_relay(0), far_relay(64)]
    gather_relay(w_g[1], *w_pieces(1))
    for d in range(4):
        zd = turn(zl, 4 - d)
        rings[d][0].wait_recv()
        rings[d].append(same(stack.at[turn(y, 3) * 4 + zd, lo], group=to_north))
        rings[d][1].wait_recv()
        rings[d].append(same(stack.at[turn(y, 1) * 4 + zd, hi], group=to_south))

    def half_pieces(start):
        return (
            lambda k: wx.at[2, k, c, pl.ds(start, 64)],
            lambda k: wx.at[2, k, c, pl.ds(start, 32)],
            lambda k: wx.at[2, k, c, pl.ds(start + 32, 32)],
        )

    def last_start(start):
        for copy in far_in[start // 64]:
            copy.wait_recv()
        rows = slice(start, start + 64)
        other = jnp.where(is_up, wn[0, rows], wn[1, rows])
        wx[2, x, c, rows] = jnp.where(last_across == 1, wf[rows], other)
        return gather_start(half_pieces(start)[0])

    w_g.append(last_start(0))

    def add_block(n, k):
        w = jnp.concatenate([decode(wx[n, k, 0]), decode(wx[n, k, 1])], axis=0)
        high, low = split(w)
        block = khl[entry[n] * 4 + k]
        both = dot(block, high)
        near[...] -= both[:ROWS] + both[ROWS:] + dot(block[:ROWS], low)

    def add_near(n):
        @pl.loop(0, 4)
        def _(k):
            add_block(n, k)

    near[...] = labels[...] - ridge[0] * coef[...]
    gather_wait(cpl_g)
    for h in range(16):
        for half in range(2):
            start = h * 256 + half * 128
            high, low = split(cplb[:, :, :, start:start + 128].reshape(64, 128))
            chl[half * 128:half * 128 + 64, h * 128:(h + 1) * 128] = high
            chl[half * 128 + 64:(half + 1) * 128, h * 128:(h + 1) * 128] = low
    gather_wait(w_g[0])
    add_near(0)
    gather_end(w_g[1], *w_pieces(1))

    for ring in rings:
        ring[2].wait_recv()
        ring[3].wait_recv()
    both = dot(chl[...], stack[...].reshape(2048, 128))
    first, second = both[:64] + both[64:128], both[128:192] + both[192:]
    block = first[:, :64] + second[:, 64:]
    cb[zh, pos] = jnp.concatenate([block[:32], block[32:]], axis=1)

    def to_row(z_):
        return [same(cb.at[z_, pos], leaf=p) for p in row_peers]

    cz = [same(cb.at[zh, pos], leaf=p) for p in (leaf_at(across, x, c), to_up, to_down)]
    cb_in = to_row(zh)
    w_g.append(last_start(64))
    gather_relay(w_g[2], *half_pieces(0))
    cz[1].wait_recv()
    cb_in += to_row(down)
    cz[2].wait_recv()
    cb_in += to_row(up)
    gather_relay(w_g[3], *half_pieces(64))
    gather_end(w_g[2], *half_pieces(0))
    gather_wait(w_g[1])
    add_near(1)
    cz[0].wait_recv()
    cb_in += to_row(across)
    gather_end(w_g[3], *half_pieces(64))
    for i, k in ((2, x), (4, left), (6, right), (7, beyond)):
        w_g[2][i].wait_recv()
        w_g[3][i].wait_recv()
        add_block(2, k)
    for copy in cb_in:
        copy.wait_recv()

    for k in range(4):
        rows = []
        for z_ in range(4):
            a, b = cb[z_, 2 * k], cb[z_, 2 * k + 1]
            rows += [
                jnp.concatenate([a[:, :64], b[:, :64]], axis=1),
                jnp.concatenate([a[:, 64:], b[:, 64:]], axis=1),
            ]
        cols = slice(k * 128, (k + 1) * 128)
        far = dot(bmat[...], jnp.concatenate(rows, axis=0), HIGHEST)
        out[0, :, cols] = near[:, cols] - far

    for copy in sent:
        copy.wait_send()


def shards(coef, labels, near_kernel, basis, transfer, coupling, lists, ridge):
    operands = coef, labels, near_kernel, basis, transfer, coupling, lists.transpose(2, 0, 1), ridge
    v = pltpu.VMEM
    hbm = pl.BlockSpec(memory_space=pltpu.HBM)
    return pl.pallas_call(
        kernel,
        out_shape=jax.ShapeDtypeStruct((1, ROWS, 512), F32),
        in_specs=[hbm] * 7 + [pl.BlockSpec(memory_space=pltpu.SMEM)],
        out_specs=pl.BlockSpec(memory_space=v),
        scratch_shapes=[
            v((ROWS, 512), F32),
            v((ROWS, 512), F32),
            v((ROWS, 256), F32),
            pltpu.SMEM((NEAR, 1, 4), jnp.int32),
            v((ROWS, 3072), F32),
            v((12, 256, 256), BF16),
            v((2, ROWS, 512), I16),
            v((ROWS, 512), I16),
            v((NEAR, 4, 2, ROWS, 512), I16),
            v((ROWS, 512), F32),
            v((256, 256), F32),
            v((ROWS, 256), F32),
            v((4, 2, 8, 4096), F32),
            v((256, 2048), BF16),
            v((4, 2, 64, 256), F32),
            v((4, 64, 256), F32),
            v((4, 128, 128), F32),
            v((4, 144, 128), I16),
            v((3, 144, 128), I16),
            v((2, 80, 128), I16),
            v((2, 80, 128), I16),
            v((2, 80, 128), I16),
            v((2, 80, 128), I16),
            v((16, 128, 128), BF16),
            v((4, 8, 32, 128), F32),
            pltpu.SemaphoreType.DMA((7,)),
            pltpu.SemaphoreType.DMA((LINKS,)),
            pltpu.SemaphoreType.DMA((LINKS,)),
        ],
        compiler_params=pltpu.CompilerParams(
            collective_id=0, has_side_effects=True, vmem_limit_bytes=67_043_328
        ),
    )(*operands)


def solution(mesh):
    split_rows = P("group", "leaf", None)
    placed = (split_rows,) * 6 + (P("group", None, None), P())
    return jax.shard_map(
        shards, mesh=mesh, in_specs=placed, out_specs=split_rows, check_vma=False
    )
```

```python
import jax
import jax.numpy as jnp
from jax import lax
from jax.experimental import pallas as pl
from jax.experimental.pallas import tpu as pltpu
from jax.sharding import PartitionSpec as P

F32 = jnp.float32
BF16 = jnp.bfloat16
I16 = jnp.int16
HIGHEST = lax.Precision.HIGHEST
MESH = pl.DeviceIdType.MESH

ROWS = 128
TOP = 6.0
NEAR = 3
LINKS = 128


def dot(a, b, precision=None, dims=((1,), (0,))):
    return lax.dot_general(a, b, (dims, ((), ())), precision=precision, preferred_element_type=F32)


def split(a):
    high = a.astype(BF16)
    return high, (a - high.astype(F32)).astype(BF16)


def encode(w):
    root = jnp.sqrt(jnp.sqrt(jnp.minimum(jnp.abs(w) * (1.0 / TOP), 1.0)))
    return jnp.round(jnp.where(w < 0, -32767.0, 32767.0) * root).astype(jnp.int32).astype(I16)


def decode(codes):
    root = codes.astype(jnp.int32).astype(F32) * (1.0 / 32767.0)
    square = root * root
    return jnp.where(root < 0, -TOP, TOP) * (square * square)


def pack(v):
    peak = jnp.maximum(jnp.max(jnp.abs(v), axis=0, keepdims=True), 1e-30)
    exponent = jnp.ceil(jnp.log2(peak) + 1e-3)
    codes = jnp.clip(jnp.round(v * (jnp.exp2(-exponent) * 32767.0)), -32767.0, 32767.0)
    both = jnp.concatenate([codes, jnp.broadcast_to(exponent, (16, v.shape[1]))], axis=0)
    return both.astype(jnp.int32).astype(I16)


def unpack(coded):
    v = coded.astype(jnp.int32).astype(F32)
    return v[:-16] * (jnp.exp2(v[-16:-15]) * (1.0 / 32767.0))


def kernel(
    coef_in, labels_in, near_kernel, basis_in, transfer, coupling, lists_in, ridge, out,
    coef, labels, basis, lists, kraw, khl, wn, wf, wx, near, efull, bz, acc, cplb, chl,
    pt, pgot, hx, hc, rs, c1, r1, c2, r2, stack, cb, lsem, ssem, rsem,
):
    me = lax.axis_index("leaf")
    g = lax.axis_index("group")
    zh = me // 8
    pos = lax.rem(me, 8)
    x = pos // 2
    c = lax.rem(pos, 2)
    oc = 1 - c
    y = g // 4
    zl = lax.rem(g, 4)

    def turn(i, d):
        return lax.rem(i + d, 4)

    up, down, across = turn(zh, 1), turn(zh, 3), turn(zh, 2)
    right, left, beyond = turn(x, 1), turn(x, 3), turn(x, 2)

    def leaf_at(z_, x_, c_):
        return z_ * 8 + x_ * 2 + c_

    to_right, to_left = leaf_at(zh, right, c), leaf_at(zh, left, c)
    to_up, to_down = leaf_at(up, x, c), leaf_at(down, x, c)
    partner = leaf_at(zh, x, oc)
    row_peers = [zh * 8 + lax.rem(pos + d, 8) for d in (4, 3, 5, 2, 6, 1, 7)]
    run_peers = [y * 4 + turn(zl, d) for d in range(1, 4)]
    to_north, to_south = turn(y, 1) * 4 + zl, turn(y, 3) * 4 + zl

    sent = []

    def send(src, dst, leaf=None, group=None):
        i = len(sent)
        target = {"leaf": leaf} if group is None else {"group": group}
        copy = pltpu.make_async_remote_copy(
            src_ref=src, dst_ref=dst, send_sem=ssem.at[i], recv_sem=rsem.at[i],
            device_id=target, device_id_type=MESH,
        )
        copy.start()
        sent.append(copy)
        return copy

    def same(ref, leaf=None, group=None):
        return send(ref, ref, leaf, group)

    own_rows = pl.ds(pl.multiple_of(pos * 32, 32), 32)
    loads = [
        pltpu.make_async_copy(src, dst, lsem.at[i])
        for i, (src, dst) in enumerate([
            (coef_in.at[0], coef), (basis_in.at[0], basis), (transfer.at[0], efull.at[own_rows, :]),
            (coupling.at[0], cplb.at[x, c]), (near_kernel.at[0], kraw), (labels_in.at[0], labels),
            (lists_in, lists),
        ])
    ]
    for load in loads:
        load.start()

    barrier = pltpu.get_barrier_semaphore()
    for peer in row_peers + [to_up, to_down]:
        pl.semaphore_signal(barrier, inc=1, device_id={"leaf": peer}, device_id_type=MESH)
    for peer in run_peers + [to_north, to_south]:
        pl.semaphore_signal(barrier, inc=1, device_id={"group": peer}, device_id_type=MESH)

    loads[0].wait()
    loads[1].wait()
    part = dot(coef[...], basis[...], HIGHEST, ((0,), (0,)))
    for k in range(4):
        for h in range(2):
            pt[k, h] = part[(2 * k + h) * 64:(2 * k + h + 1) * 64]
    wx[0, x, c] = encode(coef[...])
    loads[2].wait()
    pl.semaphore_wait(barrier, len(row_peers) + len(run_peers) + 4)

    core_sum = send(pt.at[:, oc], pgot, leaf=partner)

    def gather_start(piece):
        return [same(piece(x), leaf=p) for p in (to_right, to_left, partner)]

    def gather_relay(copies, piece, first, second):
        copies[0].wait_recv()
        copies += [same(first(left), leaf=to_right), same(piece(left), leaf=partner)]
        copies[1].wait_recv()
        copies += [same(second(right), leaf=to_left), same(piece(right), leaf=partner)]

    def gather_end(copies, piece, *_):
        copies[3].wait_recv()
        copies[5].wait_recv()
        copies.append(same(piece(beyond), leaf=partner))

    def gather_wait(copies):
        for i in (2, 4, 6, 7):
            copies[i].wait_recv()

    def e_rows(k, start, size):
        return efull.at[pl.ds(pl.multiple_of((2 * k + c) * 32 + start, 16), size), :]

    e_pieces = (
        lambda k: e_rows(k, 0, 32), lambda k: e_rows(k, 0, 16), lambda k: e_rows(k, 16, 16)
    )
    cpl_pieces = (
        lambda k: cplb.at[k, c],
        lambda k: cplb.at[k, c, :, pl.ds(0, 2048)],
        lambda k: cplb.at[k, c, :, pl.ds(2048, 2048)],
    )

    def w_pieces(n):
        return (
            lambda k: wx.at[n, k, c],
            lambda k: wx.at[n, k, c, pl.ds(0, 64)],
            lambda k: wx.at[n, k, c, pl.ds(64, 64)],
        )

    e_g = gather_start(e_pieces[0])
    w_in = [
        send(wx.at[0, x, c, pl.ds(0, 64)], wn.at[0, pl.ds(0, 64)], leaf=to_up),
        send(wx.at[0, x, c, pl.ds(0, 64)], wn.at[1, pl.ds(0, 64)], leaf=to_down),
    ]
    core_sum.wait_recv()
    for k in range(4):
        both = pt[k, c] + pgot[k]
        hx[k] = jnp.concatenate([both[:, :128], both[:, 128:]], axis=0)
        hc[k] = pack(hx[k])
    rs_in = [
        send(hc.at[turn(x, d)], rs.at[d - 1], leaf=leaf_at(zh, turn(x, d), c)) for d in range(1, 4)
    ]
    gather_relay(e_g, *e_pieces)
    loads[3].wait()
    cpl_g = gather_start(cpl_pieces[0])
    w_g = [gather_start(w_pieces(0)[0])]
    gather_end(e_g, *e_pieces)
    gather_wait(e_g)

    for copy in rs_in:
        copy.wait_recv()
    total = (hx[x] + unpack(rs[0])) + (unpack(rs[1]) + unpack(rs[2]))
    total = jnp.concatenate([total[:64], total[64:]], axis=1)
    group = dot(total, efull[...], HIGHEST).T
    group = jnp.concatenate([group[:128], group[128:]], axis=1)
    c1[0], c1[1] = pack(group[:64]), pack(group[64:])
    near_z, other_z = leaf_at(zh + 1 - 2 * lax.rem(zh, 2), x, c), leaf_at(3 - zh, x, c)
    lo, hi = pl.ds(0, 64), pl.ds(64, 64)
    ar = [
        send(c1.at[0], r1.at[0], leaf=near_z),
        send(c1.at[1], r1.at[1], leaf=other_z),
    ]
    w_in += [
        send(wx.at[0, x, c, pl.ds(64, 32)], wn.at[0, pl.ds(64, 32)], leaf=to_up),
        send(wx.at[0, x, c, pl.ds(64, 32)], wn.at[1, pl.ds(64, 32)], leaf=to_down),
    ]
    high, low = split(dot(basis[...], efull[...], HIGHEST))
    for z_ in range(4):
        bz[z_, :ROWS] = high[:, z_ * 64:(z_ + 1) * 64]
        bz[z_, ROWS:] = low[:, z_ * 64:(z_ + 1) * 64]
    for load in loads[4:]:
        load.wait()

    @pl.loop(0, 12)
    def _(b):
        high, low = split(kraw[:, pl.ds(pl.multiple_of(b * 256, 256), 256)])
        khl[b, :ROWS] = high
        khl[b, ROWS:] = low

    gather_relay(cpl_g, *cpl_pieces)
    gather_relay(w_g[0], *w_pieces(0))
    ar[0].wait_recv()
    ar[1].wait_recv()
    for h in range(2):
        c2[h] = pack(unpack(c1[h]) + unpack(r1[h]))
    ar += [
        send(c2.at[0], r2.at[0], leaf=other_z),
        send(c2.at[1], r2.at[1], leaf=near_z),
    ]

    def far_relay(start):
        first, second = pl.ds(start, 32), pl.ds(start + 32, 32)
        return [
            send(wn.at[0, first], wf.at[first], leaf=to_up),
            send(wn.at[1, second], wf.at[second], leaf=to_down),
        ]

    w_in += [
        send(wx.at[0, x, c, pl.ds(96, 32)], wn.at[0, pl.ds(96, 32)], leaf=to_up),
        send(wx.at[0, x, c, pl.ds(96, 32)], wn.at[1, pl.ds(96, 32)], leaf=to_down),
    ]
    for copy in w_in[:2]:
        copy.wait_recv()
    one, two = lists[1, 0, zh], lists[2, 0, zh]
    one_adjacent = lax.rem(one + zh, 2)
    adjacent = one_adjacent * one + (1 - one_adjacent) * two
    last = one + two - adjacent
    last_across = 1 - lax.rem(last + zh, 2)
    entry = [0, 2 - one_adjacent, 1 + one_adjacent]
    is_up = lax.rem(adjacent + 4 - zh, 4) == 1
    gather_end(w_g[0], *w_pieces(0))
    gather_end(cpl_g, *cpl_pieces)
    gather_wait(cpl_g)
    for h in range(16):
        for half in range(2):
            start = h * 256 + half * 128
            high, low = split(cplb[:, :, :, start:start + 128].reshape(64, 128))
            chl[half * 128:half * 128 + 64, h * 128:(h + 1) * 128] = high
            chl[half * 128 + 64:(half + 1) * 128, h * 128:(h + 1) * 128] = low

    ar[2].wait_recv()
    ar[3].wait_recv()
    for h in range(2):
        stack[g, 64 * h:64 * (h + 1)] = (unpack(c2[h]) + unpack(r2[h])).astype(BF16)
    runs = [same(stack.at[g], group=p) for p in run_peers]
    rings = [[same(stack.at[g], group=to_north), same(stack.at[g], group=to_south)]]
    for copy in w_in[2:]:
        copy.wait_recv()
    wx[1, x, c] = jnp.where(is_up, wn[1], wn[0])
    w_g.append(gather_start(w_pieces(1)[0]))
    for d in range(1, 4):
        runs[d - 1].wait_recv()
        ref = stack.at[y * 4 + turn(zl, 4 - d)]
        rings.append([same(ref, group=to_north), same(ref, group=to_south)])
    far_in = [far_relay(0), far_relay(64)]

    def coupled(y_):
        span = pl.ds(pl.multiple_of(y_ * 512, 512), 512)
        return dot(chl[:, span], stack[pl.ds(y_ * 4, 4)].reshape(512, 128))

    acc[...] = coupled(y)
    gather_relay(w_g[1], *w_pieces(1))
    for d in range(4):
        zd = turn(zl, 4 - d)
        rings[d][0].wait_recv()
        rings[d].append(same(stack.at[turn(y, 3) * 4 + zd, lo], group=to_north))
        rings[d][1].wait_recv()
        rings[d].append(same(stack.at[turn(y, 1) * 4 + zd, hi], group=to_south))
    acc[...] += coupled(turn(y, 1)) + coupled(turn(y, 3))

    def half_pieces(start):
        return (
            lambda k: wx.at[2, k, c, pl.ds(start, 64)],
            lambda k: wx.at[2, k, c, pl.ds(start, 32)],
            lambda k: wx.at[2, k, c, pl.ds(start + 32, 32)],
        )

    def last_start(start):
        for copy in far_in[start // 64]:
            copy.wait_recv()
        rows = slice(start, start + 64)
        other = jnp.where(is_up, wn[0, rows], wn[1, rows])
        wx[2, x, c, rows] = jnp.where(last_across == 1, wf[rows], other)
        return gather_start(half_pieces(start)[0])

    w_g.append(last_start(0))

    def add_block(n, k):
        w = jnp.concatenate([decode(wx[n, k, 0]), decode(wx[n, k, 1])], axis=0)
        high, low = split(w)
        block = khl[entry[n] * 4 + k]
        both = dot(block, high)
        near[...] -= both[:ROWS] + both[ROWS:] + dot(block[:ROWS], low)

    def add_near(n):
        @pl.loop(0, 4)
        def _(k):
            add_block(n, k)

    near[...] = labels[...] - ridge[0] * coef[...]
    gather_wait(w_g[0])
    add_near(0)
    gather_end(w_g[1], *w_pieces(1))

    for ring in rings:
        ring[2].wait_recv()
        ring[3].wait_recv()
    both = acc[...] + coupled(turn(y, 2))
    first, second = both[:64] + both[64:128], both[128:192] + both[192:]
    block = first[:, :64] + second[:, 64:]
    cb[zh, pos] = jnp.concatenate([block[:32], block[32:]], axis=1)

    def to_row(z_):
        return [same(cb.at[z_, pos], leaf=p) for p in row_peers]

    cz = [same(cb.at[zh, pos], leaf=p) for p in (leaf_at(across, x, c), to_up, to_down)]
    cb_own = to_row(zh)
    w_g.append(last_start(64))
    gather_relay(w_g[2], *half_pieces(0))
    cz[1].wait_recv()
    cb_down = to_row(down)
    cz[2].wait_recv()
    cb_up = to_row(up)
    gather_relay(w_g[3], *half_pieces(64))
    gather_end(w_g[2], *half_pieces(0))
    gather_wait(w_g[1])
    add_near(1)

    def far_part(copies, z_):
        for copy in copies:
            copy.wait_recv()
        cols = []
        for k in range(4):
            a, b = cb[z_, 2 * k], cb[z_, 2 * k + 1]
            cols.append(jnp.concatenate([
                jnp.concatenate([a[:, :64], b[:, :64]], axis=1),
                jnp.concatenate([a[:, 64:], b[:, 64:]], axis=1),
            ], axis=0))
        high, low = split(jnp.concatenate(cols, axis=1))
        both = dot(bz[z_], high)
        return both[:ROWS] + both[ROWS:] + dot(bz[z_, :ROWS], low)

    near[...] -= far_part(cb_own, zh)
    cz[0].wait_recv()
    cb_across = to_row(across)
    gather_end(w_g[3], *half_pieces(64))
    near[...] -= far_part(cb_down, down)
    near[...] -= far_part(cb_up, up)
    for i, k in ((2, x), (4, left), (6, right), (7, beyond)):
        w_g[2][i].wait_recv()
        w_g[3][i].wait_recv()
        add_block(2, k)
    out[0] = near[...] - far_part(cb_across, across)

    for copy in sent:
        copy.wait_send()


def shards(coef, labels, near_kernel, basis, transfer, coupling, lists, ridge):
    operands = coef, labels, near_kernel, basis, transfer, coupling, lists.transpose(2, 0, 1)
    operands = [pltpu.with_memory_space_constraint(a, pltpu.HBM) for a in operands]
    v = pltpu.VMEM
    hbm = pl.BlockSpec(memory_space=pltpu.HBM)
    return pl.pallas_call(
        kernel,
        out_shape=jax.ShapeDtypeStruct((1, ROWS, 512), F32),
        in_specs=[hbm] * 7 + [pl.BlockSpec(memory_space=pltpu.SMEM)],
        out_specs=pl.BlockSpec(memory_space=v),
        scratch_shapes=[
            v((ROWS, 512), F32),
            v((ROWS, 512), F32),
            v((ROWS, 256), F32),
            pltpu.SMEM((NEAR, 1, 4), jnp.int32),
            v((ROWS, 3072), F32),
            v((12, 256, 256), BF16),
            v((2, ROWS, 512), I16),
            v((ROWS, 512), I16),
            v((NEAR, 4, 2, ROWS, 512), I16),
            v((ROWS, 512), F32),
            v((256, 256), F32),
            v((4, 256, 64), BF16),
            v((256, 128), F32),
            v((4, 2, 8, 4096), F32),
            v((256, 2048), BF16),
            v((4, 2, 64, 256), F32),
            v((4, 64, 256), F32),
            v((4, 128, 128), F32),
            v((4, 144, 128), I16),
            v((3, 144, 128), I16),
            v((2, 80, 128), I16),
            v((2, 80, 128), I16),
            v((2, 80, 128), I16),
            v((2, 80, 128), I16),
            v((16, 128, 128), BF16),
            v((4, 8, 32, 128), F32),
            pltpu.SemaphoreType.DMA((7,)),
            pltpu.SemaphoreType.DMA((LINKS,)),
            pltpu.SemaphoreType.DMA((LINKS,)),
        ],
        compiler_params=pltpu.CompilerParams(
            collective_id=0, has_side_effects=True, vmem_limit_bytes=40 * 1024 * 1024
        ),
    )(*operands, ridge)


def solution(mesh):
    split_rows = P("group", "leaf", None)
    placed = (split_rows,) * 6 + (P("group", None, None), P())
    return jax.shard_map(
        shards, mesh=mesh, in_specs=placed, out_specs=split_rows, check_vma=False
    )
```

```python
import jax
import jax.numpy as jnp
from jax import lax
from jax.experimental import pallas as pl
from jax.experimental.pallas import tpu as pltpu
from jax.sharding import PartitionSpec as P

F32 = jnp.float32
BF16 = jnp.bfloat16
I16 = jnp.int16
HIGHEST = lax.Precision.HIGHEST
MESH = pl.DeviceIdType.MESH

ROWS = 128
TOP = 6.0
NEAR = 3
LINKS = 128


def dot(a, b, precision=None, dims=((1,), (0,))):
    return lax.dot_general(a, b, (dims, ((), ())), precision=precision, preferred_element_type=F32)


def split(a):
    high = a.astype(BF16)
    return high, (a - high.astype(F32)).astype(BF16)


def dot3(a, b, dims=((1,), (0,))):
    (a_high, a_low), (b_high, b_low) = split(a), split(b)
    small = dot(a_low, b_high, None, dims) + dot(a_high, b_low, None, dims)
    return dot(a_high, b_high, None, dims) + small


def encode(w):
    root = jnp.sqrt(jnp.sqrt(jnp.minimum(jnp.abs(w) * (1.0 / TOP), 1.0)))
    return jnp.round(jnp.where(w < 0, -32767.0, 32767.0) * root).astype(jnp.int32).astype(I16)


def decode(codes):
    root = codes.astype(jnp.int32).astype(F32) * (1.0 / 32767.0)
    square = root * root
    return jnp.where(root < 0, -TOP, TOP) * (square * square)


def pack(v):
    peak = jnp.maximum(jnp.max(jnp.abs(v), axis=0, keepdims=True), 1e-30)
    exponent = jnp.ceil(jnp.log2(peak) + 1e-3)
    codes = jnp.clip(jnp.round(v * (jnp.exp2(-exponent) * 32767.0)), -32767.0, 32767.0)
    both = jnp.concatenate([codes, jnp.broadcast_to(exponent, (16, v.shape[1]))], axis=0)
    return both.astype(jnp.int32).astype(I16)


def unpack(coded):
    v = coded.astype(jnp.int32).astype(F32)
    return v[:-16] * (jnp.exp2(v[-16:-15]) * (1.0 / 32767.0))


def kernel(
    coef_in, labels_in, near_kernel, basis_in, transfer, coupling, lists_in, ridge, out,
    coef, labels, basis, lists, kraw, khl, wn, wf, wx, near, efull, bz, acc, cplb, chl,
    pt, pgot, hx, hc, rs, c1, r1, c2, r2, stack, cb, lsem, ssem, rsem,
):
    me = lax.axis_index("leaf")
    g = lax.axis_index("group")
    zh = me // 8
    pos = lax.rem(me, 8)
    x = pos // 2
    c = lax.rem(pos, 2)
    oc = 1 - c
    y = g // 4
    zl = lax.rem(g, 4)

    def turn(i, d):
        return lax.rem(i + d, 4)

    up, down, across = turn(zh, 1), turn(zh, 3), turn(zh, 2)
    right, left, beyond = turn(x, 1), turn(x, 3), turn(x, 2)

    def leaf_at(z_, x_, c_):
        return z_ * 8 + x_ * 2 + c_

    to_right, to_left = leaf_at(zh, right, c), leaf_at(zh, left, c)
    to_up, to_down = leaf_at(up, x, c), leaf_at(down, x, c)
    partner = leaf_at(zh, x, oc)
    row_peers = [zh * 8 + lax.rem(pos + d, 8) for d in (4, 3, 5, 2, 6, 1, 7)]
    run_peers = [y * 4 + turn(zl, d) for d in range(1, 4)]
    to_north, to_south = turn(y, 1) * 4 + zl, turn(y, 3) * 4 + zl

    sent = []

    def send(src, dst, leaf=None, group=None):
        i = len(sent)
        target = {"leaf": leaf} if group is None else {"group": group}
        copy = pltpu.make_async_remote_copy(
            src_ref=src, dst_ref=dst, send_sem=ssem.at[i], recv_sem=rsem.at[i],
            device_id=target, device_id_type=MESH,
        )
        copy.start()
        sent.append(copy)
        return copy

    def same(ref, leaf=None, group=None):
        return send(ref, ref, leaf, group)

    own_rows = pl.ds(pl.multiple_of(pos * 32, 32), 32)
    loads = [
        pltpu.make_async_copy(src, dst, lsem.at[i])
        for i, (src, dst) in enumerate([
            (coef_in.at[0], coef), (basis_in.at[0], basis), (transfer.at[0], efull.at[own_rows, :]),
            (coupling.at[0], cplb.at[x, c]), (near_kernel.at[0], kraw), (labels_in.at[0], labels),
            (lists_in, lists),
        ])
    ]
    for load in loads:
        load.start()

    barrier = pltpu.get_barrier_semaphore()
    for peer in row_peers + [to_up, to_down]:
        pl.semaphore_signal(barrier, inc=1, device_id={"leaf": peer}, device_id_type=MESH)
    for peer in run_peers + [to_north, to_south]:
        pl.semaphore_signal(barrier, inc=1, device_id={"group": peer}, device_id_type=MESH)

    loads[0].wait()
    loads[1].wait()
    part = dot3(coef[...], basis[...], ((0,), (0,)))
    for k in range(4):
        for h in range(2):
            pt[k, h] = part[(2 * k + h) * 64:(2 * k + h + 1) * 64]
    wx[0, x, c] = encode(coef[...])
    loads[2].wait()
    pl.semaphore_wait(barrier, len(row_peers) + len(run_peers) + 4)

    core_sum = send(pt.at[:, oc], pgot, leaf=partner)

    def gather_start(piece):
        return [same(piece(x), leaf=p) for p in (to_right, to_left, partner)]

    def gather_relay(copies, piece, first, second):
        copies[0].wait_recv()
        copies += [same(first(left), leaf=to_right), same(piece(left), leaf=partner)]
        copies[1].wait_recv()
        copies += [same(second(right), leaf=to_left), same(piece(right), leaf=partner)]

    def gather_end(copies, piece, *_):
        copies[3].wait_recv()
        copies[5].wait_recv()
        copies.append(same(piece(beyond), leaf=partner))

    def gather_wait(copies):
        for i in (2, 4, 6, 7):
            copies[i].wait_recv()

    def e_rows(k, start, size):
        return efull.at[pl.ds(pl.multiple_of((2 * k + c) * 32 + start, 16), size), :]

    e_pieces = (
        lambda k: e_rows(k, 0, 32), lambda k: e_rows(k, 0, 16), lambda k: e_rows(k, 16, 16)
    )
    cpl_pieces = (
        lambda k: cplb.at[k, c],
        lambda k: cplb.at[k, c, :, pl.ds(0, 2048)],
        lambda k: cplb.at[k, c, :, pl.ds(2048, 2048)],
    )

    def w_pieces(n):
        return (
            lambda k: wx.at[n, k, c],
            lambda k: wx.at[n, k, c, pl.ds(0, 64)],
            lambda k: wx.at[n, k, c, pl.ds(64, 64)],
        )

    e_g = gather_start(e_pieces[0])
    w_in = [
        send(wx.at[0, x, c, pl.ds(0, 64)], wn.at[0, pl.ds(0, 64)], leaf=to_up),
        send(wx.at[0, x, c, pl.ds(0, 64)], wn.at[1, pl.ds(0, 64)], leaf=to_down),
    ]
    core_sum.wait_recv()
    for k in range(4):
        both = pt[k, c] + pgot[k]
        hx[k] = jnp.concatenate([both[:, :128], both[:, 128:]], axis=0)
        hc[k] = pack(hx[k])
    rs_in = [
        send(hc.at[turn(x, d)], rs.at[d - 1], leaf=leaf_at(zh, turn(x, d), c)) for d in range(1, 4)
    ]
    gather_relay(e_g, *e_pieces)
    loads[3].wait()
    cpl_g = gather_start(cpl_pieces[0])
    w_g = [gather_start(w_pieces(0)[0])]
    gather_end(e_g, *e_pieces)
    gather_wait(e_g)

    for copy in rs_in:
        copy.wait_recv()
    total = (hx[x] + unpack(rs[0])) + (unpack(rs[1]) + unpack(rs[2]))
    total = jnp.concatenate([total[:64], total[64:]], axis=1)
    group = dot3(total, efull[...]).T
    group = jnp.concatenate([group[:128], group[128:]], axis=1)
    c1[0], c1[1] = pack(group[:64]), pack(group[64:])
    near_z, other_z = leaf_at(zh + 1 - 2 * lax.rem(zh, 2), x, c), leaf_at(3 - zh, x, c)
    lo, hi = pl.ds(0, 64), pl.ds(64, 64)
    ar = [
        send(c1.at[0], r1.at[0], leaf=near_z),
        send(c1.at[1], r1.at[1], leaf=other_z),
    ]
    w_in += [
        send(wx.at[0, x, c, pl.ds(64, 32)], wn.at[0, pl.ds(64, 32)], leaf=to_up),
        send(wx.at[0, x, c, pl.ds(64, 32)], wn.at[1, pl.ds(64, 32)], leaf=to_down),
    ]
    high, low = split(dot(basis[...], efull[...], HIGHEST))
    for z_ in range(4):
        bz[z_, :ROWS] = high[:, z_ * 64:(z_ + 1) * 64]
        bz[z_, ROWS:] = low[:, z_ * 64:(z_ + 1) * 64]
    for load in loads[4:]:
        load.wait()

    @pl.loop(0, 12)
    def _(b):
        high, low = split(kraw[:, pl.ds(pl.multiple_of(b * 256, 256), 256)])
        khl[b, :ROWS] = high
        khl[b, ROWS:] = low

    gather_relay(cpl_g, *cpl_pieces)
    gather_relay(w_g[0], *w_pieces(0))
    ar[0].wait_recv()
    ar[1].wait_recv()
    for h in range(2):
        c2[h] = pack(unpack(c1[h]) + unpack(r1[h]))
    ar += [
        send(c2.at[0], r2.at[0], leaf=other_z),
        send(c2.at[1], r2.at[1], leaf=near_z),
    ]

    def far_relay(start):
        first, second = pl.ds(start, 32), pl.ds(start + 32, 32)
        return [
            send(wn.at[0, first], wf.at[first], leaf=to_up),
            send(wn.at[1, second], wf.at[second], leaf=to_down),
        ]

    w_in += [
        send(wx.at[0, x, c, pl.ds(96, 32)], wn.at[0, pl.ds(96, 32)], leaf=to_up),
        send(wx.at[0, x, c, pl.ds(96, 32)], wn.at[1, pl.ds(96, 32)], leaf=to_down),
    ]
    for copy in w_in[:2]:
        copy.wait_recv()
    one, two = lists[1, 0, zh], lists[2, 0, zh]
    one_adjacent = lax.rem(one + zh, 2)
    adjacent = one_adjacent * one + (1 - one_adjacent) * two
    last = one + two - adjacent
    last_across = 1 - lax.rem(last + zh, 2)
    entry = [0, 2 - one_adjacent, 1 + one_adjacent]
    is_up = lax.rem(adjacent + 4 - zh, 4) == 1
    gather_end(w_g[0], *w_pieces(0))
    gather_end(cpl_g, *cpl_pieces)
    gather_wait(cpl_g)
    for h in range(16):
        for half in range(2):
            start = h * 256 + half * 128
            high, low = split(cplb[:, :, :, start:start + 128].reshape(64, 128))
            chl[half * 128:half * 128 + 64, h * 128:(h + 1) * 128] = high
            chl[half * 128 + 64:(half + 1) * 128, h * 128:(h + 1) * 128] = low

    ar[2].wait_recv()
    ar[3].wait_recv()
    for h in range(2):
        stack[g, 64 * h:64 * (h + 1)] = (unpack(c2[h]) + unpack(r2[h])).astype(BF16)
    runs = [same(stack.at[g], group=p) for p in run_peers]
    rings = [[same(stack.at[g], group=to_north), same(stack.at[g], group=to_south)]]
    for copy in w_in[2:]:
        copy.wait_recv()
    wx[1, x, c] = jnp.where(is_up, wn[1], wn[0])
    w_g.append(gather_start(w_pieces(1)[0]))
    for d in range(1, 4):
        runs[d - 1].wait_recv()
        ref = stack.at[y * 4 + turn(zl, 4 - d)]
        rings.append([same(ref, group=to_north), same(ref, group=to_south)])
    far_in = [far_relay(0), far_relay(64)]

    def coupled(y_):
        span = pl.ds(pl.multiple_of(y_ * 512, 512), 512)
        return dot(chl[:, span], stack[pl.ds(y_ * 4, 4)].reshape(512, 128))

    acc[...] = coupled(y)
    gather_relay(w_g[1], *w_pieces(1))
    for d in range(4):
        zd = turn(zl, 4 - d)
        rings[d][0].wait_recv()
        rings[d].append(same(stack.at[turn(y, 3) * 4 + zd, lo], group=to_north))
        rings[d][1].wait_recv()
        rings[d].append(same(stack.at[turn(y, 1) * 4 + zd, hi], group=to_south))
    acc[...] += coupled(turn(y, 1)) + coupled(turn(y, 3))

    def half_pieces(start):
        return (
            lambda k: wx.at[2, k, c, pl.ds(start, 64)],
            lambda k: wx.at[2, k, c, pl.ds(start, 32)],
            lambda k: wx.at[2, k, c, pl.ds(start + 32, 32)],
        )

    def last_start(start):
        for copy in far_in[start // 64]:
            copy.wait_recv()
        rows = slice(start, start + 64)
        other = jnp.where(is_up, wn[0, rows], wn[1, rows])
        wx[2, x, c, rows] = jnp.where(last_across == 1, wf[rows], other)
        return gather_start(half_pieces(start)[0])

    w_g.append(last_start(0))

    def add_block(n, k):
        w = jnp.concatenate([decode(wx[n, k, 0]), decode(wx[n, k, 1])], axis=0)
        high, low = split(w)
        block = khl[entry[n] * 4 + k]
        both = dot(block, high)
        near[...] -= both[:ROWS] + both[ROWS:] + dot(block[:ROWS], low)

    def add_near(n):
        @pl.loop(0, 4)
        def _(k):
            add_block(n, k)

    near[...] = labels[...] - ridge[0] * coef[...]
    gather_wait(w_g[0])
    add_near(0)
    gather_end(w_g[1], *w_pieces(1))

    for ring in rings:
        ring[2].wait_recv()
        ring[3].wait_recv()
    both = acc[...] + coupled(turn(y, 2))
    first, second = both[:64] + both[64:128], both[128:192] + both[192:]
    block = first[:, :64] + second[:, 64:]
    cb[zh, pos] = jnp.concatenate([block[:32], block[32:]], axis=1)

    def to_row(z_):
        return [same(cb.at[z_, pos], leaf=p) for p in row_peers]

    cz = [same(cb.at[zh, pos], leaf=p) for p in (leaf_at(across, x, c), to_up, to_down)]
    cb_own = to_row(zh)
    w_g.append(last_start(64))
    gather_relay(w_g[2], *half_pieces(0))
    cz[1].wait_recv()
    cb_down = to_row(down)
    cz[2].wait_recv()
    cb_up = to_row(up)
    gather_relay(w_g[3], *half_pieces(64))
    gather_end(w_g[2], *half_pieces(0))
    gather_wait(w_g[1])
    add_near(1)

    def far_part(copies, z_):
        for copy in copies:
            copy.wait_recv()
        cols = []
        for k in range(4):
            a, b = cb[z_, 2 * k], cb[z_, 2 * k + 1]
            cols.append(jnp.concatenate([
                jnp.concatenate([a[:, :64], b[:, :64]], axis=1),
                jnp.concatenate([a[:, 64:], b[:, 64:]], axis=1),
            ], axis=0))
        high, low = split(jnp.concatenate(cols, axis=1))
        both = dot(bz[z_], high)
        return both[:ROWS] + both[ROWS:] + dot(bz[z_, :ROWS], low)

    near[...] -= far_part(cb_own, zh)
    cz[0].wait_recv()
    cb_across = to_row(across)
    gather_end(w_g[3], *half_pieces(64))
    near[...] -= far_part(cb_down, down)
    near[...] -= far_part(cb_up, up)
    for i, k in ((2, x), (4, left), (6, right), (7, beyond)):
        w_g[2][i].wait_recv()
        w_g[3][i].wait_recv()
        add_block(2, k)
    out[0] = near[...] - far_part(cb_across, across)

    for copy in sent:
        copy.wait_send()


def shards(coef, labels, near_kernel, basis, transfer, coupling, lists, ridge):
    operands = coef, labels, near_kernel, basis, transfer, coupling, lists.transpose(2, 0, 1)
    operands = [pltpu.with_memory_space_constraint(a, pltpu.HBM) for a in operands]
    v = pltpu.VMEM
    hbm = pl.BlockSpec(memory_space=pltpu.HBM)
    return pl.pallas_call(
        kernel,
        out_shape=jax.ShapeDtypeStruct((1, ROWS, 512), F32),
        in_specs=[hbm] * 7 + [pl.BlockSpec(memory_space=pltpu.SMEM)],
        out_specs=pl.BlockSpec(memory_space=v),
        scratch_shapes=[
            v((ROWS, 512), F32),
            v((ROWS, 512), F32),
            v((ROWS, 256), F32),
            pltpu.SMEM((NEAR, 1, 4), jnp.int32),
            v((ROWS, 3072), F32),
            v((12, 256, 256), BF16),
            v((2, ROWS, 512), I16),
            v((ROWS, 512), I16),
            v((NEAR, 4, 2, ROWS, 512), I16),
            v((ROWS, 512), F32),
            v((256, 256), F32),
            v((4, 256, 64), BF16),
            v((256, 128), F32),
            v((4, 2, 8, 4096), F32),
            v((256, 2048), BF16),
            v((4, 2, 64, 256), F32),
            v((4, 64, 256), F32),
            v((4, 128, 128), F32),
            v((4, 144, 128), I16),
            v((3, 144, 128), I16),
            v((2, 80, 128), I16),
            v((2, 80, 128), I16),
            v((2, 80, 128), I16),
            v((2, 80, 128), I16),
            v((16, 128, 128), BF16),
            v((4, 8, 32, 128), F32),
            pltpu.SemaphoreType.DMA((7,)),
            pltpu.SemaphoreType.DMA((LINKS,)),
            pltpu.SemaphoreType.DMA((LINKS,)),
        ],
        compiler_params=pltpu.CompilerParams(
            collective_id=0, has_side_effects=True, vmem_limit_bytes=40 * 1024 * 1024
        ),
    )(*operands, ridge)


def solution(mesh):
    split_rows = P("group", "leaf", None)
    placed = (split_rows,) * 6 + (P("group", None, None), P())
    return jax.shard_map(
        shards, mesh=mesh, in_specs=placed, out_specs=split_rows, check_vma=False
    )
```
